512 devices in a mesh: head: 8 (over y), leaf: 64 (over z, x, core).
Axes of the slice: x: 4, y: 8, z: 8, core: 2. Of those that a mesh axis runs over, the one named last changes fastest.
Arguments:
- queries: bfloat16 [128, 128, 8192], P('leaf', None, 'head'), may hold values from -6 to 6
- keys: bfloat16 [128, 128, 1024], P('leaf', 'head'), may hold values from -6 to 6
- values: bfloat16 [128, 128, 1024], P('leaf', 'head'), may hold values from -6 to 6
- output_gradient: bfloat16 [128, 128, 8192], P('leaf', None, 'head'), may hold values from -6 to 6
- parents: int32 [128], P('leaf'), may hold values from -1 to 127, as said below
Outputs:
- grad_queries: bfloat16 [128, 128, 8192], P('leaf', None, 'head')
- key_gradient: bfloat16 [128, 128, 1024], P('leaf', 'head')
- value_gradient: bfloat16 [128, 128, 1024], P('leaf', 'head')
The draws below stay inside these ranges and needn't reach their ends.
Inputs may be any that keep to these rules, and one draw needn't show every extreme that they name: `parents`: block b is in tree b % 2 and its parent is in the same tree. In the tree of even blocks the parent lies below b and only block 0 is a root; in the tree of odd blocks the parent lies above b and only block 127 is a root. Every block has at most 14 ancestors, and some block has exactly 14.
All inputs are finite; a program needn't handle non-finite values.
Results may differ from the reference program's by a relative error of at most 0.012.
Values may be sent and summed in bfloat16 or wider, within the bound.
A program may use at most 64 MiB of HBM per device.

```python
import jax
import jax.numpy as jnp
from jax import lax

QUERY_HEAD_COUNT = 64
KEY_VALUE_HEADS = 8
HEAD_DIM = 128
BLOCK_TOKENS = 128
NODE_BLOCKS = 128
MAX_ANCESTORS = 14


def grow_tree(key, count):
    hops = jax.random.randint(jax.random.fold_in(key, 1), (count,), 1, 3).astype(jnp.int32)

    def visit(state, index):
        depths, links = state
        near = (index - 1).astype(jnp.int32)

        def climb(step, node):
            return jnp.where(step < hops[index], links[node], node).astype(jnp.int32)
        lifted = lax.fori_loop(0, 2, climb, near)
        chosen = jnp.where(depths[near] < MAX_ANCESTORS, near, lifted).astype(jnp.int32)
        depths = depths.at[index].set(depths[chosen] + 1)
        links = links.at[index].set(chosen)
        return ((depths, links), chosen)
    start = (jnp.zeros((count,), jnp.int32), jnp.full((count,), -1, jnp.int32))
    _, chosen_all = lax.scan(visit, start, jnp.arange(1, count, dtype=jnp.int32))
    return jnp.concatenate([jnp.full((1,), -1, jnp.int32), chosen_all.astype(jnp.int32)])


def draw_parents(key, part):
    ranks = NODE_BLOCKS // 2
    lower = grow_tree(jax.random.fold_in(key, 31), ranks)
    upper = grow_tree(jax.random.fold_in(key, 37), ranks)
    lower_blocks = jnp.where(lower >= 0, 2 * lower, -1)
    mirrored = upper[::-1]
    upper_blocks = jnp.where(mirrored >= 0, 2 * (ranks - 1 - mirrored) + 1, -1)
    return jnp.stack([lower_blocks, upper_blocks], 1).reshape(NODE_BLOCKS).astype(jnp.int32)


def draw_queries(key, part):
    array_shape = (NODE_BLOCKS, BLOCK_TOKENS, QUERY_HEAD_COUNT * HEAD_DIM)
    draws = jnp.clip(jax.random.normal(jax.random.fold_in(key, 11), array_shape, jnp.float32), -6.0, 6.0)
    return draws.astype(jnp.bfloat16)


def draw_keys(key, part):
    array_shape = (NODE_BLOCKS, BLOCK_TOKENS, KEY_VALUE_HEADS * HEAD_DIM)
    draws = jnp.clip(jax.random.normal(jax.random.fold_in(key, 12), array_shape, jnp.float32), -6.0, 6.0)
    return draws.astype(jnp.bfloat16)


def level_of(own_key, extent, split, smallest, largest):
    factor_of, own = 1.0, jax.random.fold_in(own_key, 6)
    for position, blocks in split:
        steps = jnp.exp(jax.random.uniform(jax.random.fold_in(own, position), (blocks,), jnp.float32, smallest / len(split), largest / len(split)))
        factor_of = factor_of * jnp.repeat(steps, extent[position] // blocks).reshape([-1 if axis == position else 1 for axis in range(len(extent))])
    return factor_of


def normal_values(stream_key, dims, deviation, most, split=(), kind=jnp.bfloat16):
    values = jax.random.normal(stream_key, dims, jnp.float32) * deviation
    if len(split) > 0:
        values = level_of(stream_key, dims, split, -0.22, 0.18) * values
    return jnp.clip(values, min=-most, max=most).astype(kind)


def setup_inputs(seed: int = 0) -> dict:
    arg_keys = jax.random.split(jax.random.key(seed), 6)
    queries = draw_queries(jax.random.fold_in(arg_keys[5], 71), 0)
    keys = draw_keys(jax.random.fold_in(arg_keys[5], 71), 0)
    values = normal_values(arg_keys[2], (NODE_BLOCKS, BLOCK_TOKENS, KEY_VALUE_HEADS * HEAD_DIM), 1.0, 6.0, ((0, 64), (1, 8)))
    output_gradient = normal_values(arg_keys[3], (NODE_BLOCKS, BLOCK_TOKENS, QUERY_HEAD_COUNT * HEAD_DIM), 1.0, 6.0, ((0, 64), (2, 8)))
    parents = draw_parents(jax.random.fold_in(arg_keys[5], 71), 0)
    return {"queries": queries, "keys": keys, "values": values, "output_gradient": output_gradient, "parents": parents}


masked_score = -1.0e30


def follow_links(parent_table, chain_len):
    def extend(link_no, carry_in):
        current, ancestry = carry_in
        ancestry = ancestry.at[:, link_no].set(current)
        upward = jnp.where(current >= 0, parent_table[jnp.maximum(current, 0)], -1)
        return upward.astype(jnp.int32), ancestry
    start = jnp.full((parent_table.shape[0], chain_len), -1, jnp.int32)
    return lax.fori_loop(0, chain_len, extend, (parent_table.astype(jnp.int32), start))[1]


def reference(queries, keys, values, output_gradient, parents):
    heads_per_group = QUERY_HEAD_COUNT // KEY_VALUE_HEADS
    softmax_scale = HEAD_DIM ** -0.5
    ancestry = follow_links(parents, MAX_ANCESTORS)
    query_full = queries.astype(jnp.float32).reshape(NODE_BLOCKS, BLOCK_TOKENS, KEY_VALUE_HEADS, heads_per_group, HEAD_DIM)
    gradient_total = output_gradient.astype(jnp.float32).reshape(NODE_BLOCKS, BLOCK_TOKENS, KEY_VALUE_HEADS, heads_per_group, HEAD_DIM)
    key_full = keys.astype(jnp.float32).reshape(NODE_BLOCKS, BLOCK_TOKENS, KEY_VALUE_HEADS, HEAD_DIM)
    value_full = values.astype(jnp.float32).reshape(NODE_BLOCKS, BLOCK_TOKENS, KEY_VALUE_HEADS, HEAD_DIM)
    token_span = (MAX_ANCESTORS + 1) * BLOCK_TOKENS
    row_pos = jnp.arange(BLOCK_TOKENS, dtype=jnp.int32)[:, None]
    col_pos = jnp.arange(token_span, dtype=jnp.int32)[None, :]
    col_block = col_pos // BLOCK_TOKENS
    col_inner = col_pos % BLOCK_TOKENS

    def one_block(carry_in, index):
        key_running, value_running = carry_in
        chain = jnp.concatenate([index[None], ancestry[index]]).astype(jnp.int32)
        active = chain >= 0
        safe_value = jnp.maximum(chain, 0)
        block_keys = key_full[safe_value].reshape(token_span, KEY_VALUE_HEADS, HEAD_DIM)
        block_values = value_full[safe_value].reshape(token_span, KEY_VALUE_HEADS, HEAD_DIM)
        query_rows = query_full[index]
        grad_rows = gradient_total[index]
        visible = active[col_block] & ((col_block > 0) | (col_inner <= row_pos))
        scores = jnp.einsum("igrd,jgd->grij", query_rows, block_keys) * softmax_scale
        scores = jnp.where(visible, scores, masked_score)
        row_peak = jnp.max(scores, -1, keepdims=True)
        row_level = row_peak + jnp.log(jnp.sum(jnp.exp(scores - row_peak), -1, keepdims=True))
        weights = jnp.exp(scores - row_level)
        slopes = jnp.einsum("igrd,jgd->grij", grad_rows, block_values)
        row_mean = jnp.sum(weights * slopes, -1, keepdims=True)
        dscore = lax.optimization_barrier((weights * (slopes - row_mean)).astype(jnp.bfloat16)).astype(jnp.float32)
        rounded = lax.optimization_barrier(weights.astype(jnp.bfloat16)).astype(jnp.float32)
        query_grad = (softmax_scale * jnp.einsum("grij,jgd->igrd", dscore, block_keys)).astype(jnp.bfloat16)
        key_portion = softmax_scale * jnp.einsum("grij,igrd->jgd", dscore, query_rows)
        value_portion = jnp.einsum("grij,igrd->jgd", rounded, grad_rows)
        gate_flag = active.astype(jnp.float32)[:, None, None, None]
        key_running = key_running.at[safe_value].add(key_portion.reshape(MAX_ANCESTORS + 1, BLOCK_TOKENS, KEY_VALUE_HEADS, HEAD_DIM) * gate_flag)
        value_running = value_running.at[safe_value].add(value_portion.reshape(MAX_ANCESTORS + 1, BLOCK_TOKENS, KEY_VALUE_HEADS, HEAD_DIM) * gate_flag)
        return (key_running, value_running), query_grad.reshape(BLOCK_TOKENS, QUERY_HEAD_COUNT * HEAD_DIM)

    zero_running = jnp.zeros((NODE_BLOCKS, BLOCK_TOKENS, KEY_VALUE_HEADS, HEAD_DIM), jnp.float32)
    (key_running, value_running), query_grads = lax.scan(one_block, (zero_running, zero_running), jnp.arange(NODE_BLOCKS, dtype=jnp.int32))
    key_gradient = key_running.reshape(NODE_BLOCKS, BLOCK_TOKENS, KEY_VALUE_HEADS * HEAD_DIM).astype(jnp.bfloat16)
    value_gradient = value_running.reshape(NODE_BLOCKS, BLOCK_TOKENS, KEY_VALUE_HEADS * HEAD_DIM).astype(jnp.bfloat16)
    return query_grads, key_gradient, value_gradient
```

```python
import functools

import jax
import jax.numpy as jnp
from jax import lax
from jax.experimental import pallas as pl
from jax.experimental.pallas import tpu as pltpu
from jax.sharding import PartitionSpec as P

QUERY_HEAD_COUNT = 64
KEY_VALUE_HEADS = 8
HEAD_DIM = 128
BLOCK_TOKENS = 128
MAX_ANCESTORS = 14
HEADS_PER_GROUP = QUERY_HEAD_COUNT // KEY_VALUE_HEADS
CHAIN = MAX_ANCESTORS + 1

X_CHIPS = 4
ROW = 2 * X_CHIPS
PARENT_ROWS = 16
KV_ROWS = 2 * BLOCK_TOKENS
TILE_ROWS = KV_ROWS + PARENT_ROWS
VMEM_LIMIT = 56 * 1024 * 1024
masked_score = -1e30
MESH = pl.DeviceIdType.MESH


class Place:
    def __init__(self, heads, leaves):
        self.heads, self.layers = heads, leaves // ROW
        self.y = lax.axis_index("head")
        self.leaf = lax.axis_index("leaf")
        self.z = self.leaf // ROW
        self.x = (self.leaf % ROW) // 2
        self.core = self.leaf % 2

    def column(self, step):
        return (self.x + step + X_CHIPS) % X_CHIPS

    def leaf_of(self, z, x, core):
        return z * ROW + x * 2 + core

    def along_x(self, step):
        return (self.y, self.leaf_of(self.z, self.column(step), self.core))

    def along_z(self, step):
        return (self.y, self.leaf_of(self.z + step, self.x, self.core))

    def sibling(self):
        return (self.y, self.leaf_of(self.z, self.x, 1 - self.core))

    def head_peer(self, step):
        return ((self.y + step) % self.heads, self.leaf)

    def greet(self):
        barrier = pltpu.get_barrier_semaphore()

        def signal(device):
            pl.semaphore_signal(barrier, inc=1, device_id=device, device_id_type=MESH)

        for step in range(1, self.heads):
            signal(self.head_peer(step))
        for step in range(1, X_CHIPS):
            signal(self.along_x(step))
        signal(self.sibling())

        @pl.when(self.z > 0)
        def _():
            signal(self.along_z(-1))

        @pl.when(self.z < self.layers - 1)
        def _():
            signal(self.along_z(1))

        inner = ((self.z > 0) & (self.z < self.layers - 1)).astype(jnp.int32)
        pl.semaphore_wait(barrier, self.heads - 1 + X_CHIPS - 1 + 1 + 1 + inner)


def remote(src, dst, send_sem, recv_sem, device):
    return pltpu.make_async_remote_copy(
        src_ref=src, dst_ref=dst, send_sem=send_sem, recv_sem=recv_sem,
        device_id=device, device_id_type=MESH,
    )


def gather_kernel(
    heads, leaves, keys, values, marks, own, buf,
    y_send, y_recv, z_send, z_recv, r_send, r_recv, x_send, x_recv, h_send, h_recv,
    d_send, d_recv, e_send, e_recv,
):
    at = Place(heads, leaves)
    layers, z, x, core = at.layers, at.z, at.x, at.core
    share = BLOCK_TOKENS // heads
    at.greet()

    def regroup(step):
        column = pl.ds(pl.multiple_of(((at.y + step) % heads) * HEAD_DIM, HEAD_DIM), HEAD_DIM)
        rows_k = pl.ds(pl.multiple_of(at.y * share, share), share)
        rows_v = pl.ds(pl.multiple_of(BLOCK_TOKENS + at.y * share, share), share)
        peer = at.head_peer(step)
        return (
            remote(keys.at[:, :, column], own.at[:, rows_k, :],
                   y_send.at[2 * step], y_recv.at[2 * step], peer),
            remote(values.at[:, :, column], own.at[:, rows_v, :],
                   y_send.at[2 * step + 1], y_recv.at[2 * step + 1], peer),
        )

    for step in range(1, heads):
        for copy in regroup(step):
            copy.start()
    mine = pl.ds(pl.multiple_of(at.y * HEAD_DIM, HEAD_DIM), HEAD_DIM)
    own[:, pl.ds(pl.multiple_of(at.y * share, share), share), :] = keys[:, :, mine]
    own[:, pl.ds(pl.multiple_of(BLOCK_TOKENS + at.y * share, share), share), :] = values[:, :, mine]
    own[:, KV_ROWS:, :] = marks[...]
    for step in range(1, heads):
        for copy in regroup(step):
            copy.wait_recv()

    def slot(zz, xx, cc):
        return buf.at[zz, xx, cc]

    up_send = z_send.at[layers]
    down_send = z_send.at[layers + 1]

    def first_up():
        return remote(own.at[0], slot(z, x, core), up_send, z_recv.at[z], at.along_z(1))

    def first_down():
        return remote(own.at[1], slot(z, x, core), down_send, z_recv.at[z], at.along_z(-1))

    pl.when(z < layers - 1)(lambda: first_up().start())
    pl.when(z > 0)(lambda: first_down().start())

    def row_copy(step):
        tree = (at.column(step) < x).astype(jnp.int32)
        return remote(own.at[tree], slot(z, x, core), r_send.at[step], r_recv.at[step],
                      at.along_x(step))

    for step in (1, 3, 2):
        row_copy(step).start()

    def twin_copy():
        return remote(own.at[core], slot(z, x, core), e_send.at[0], e_recv.at[0], at.sibling())

    twin_copy().start()

    def row_from(step):
        tile = slot(z, at.column(-step), core)
        return remote(tile, tile, e_send.at[step], e_recv.at[step], at.sibling())

    def z_arrival(source):
        tile = slot(source, x, core)
        return remote(tile, tile, z_send.at[source], z_recv.at[source], at.sibling())

    def z_next(source, step):
        tile = slot(source, x, core)
        return remote(tile, tile, z_send.at[source], z_recv.at[source], at.along_z(step))

    def x_copy(source, step):
        tile = slot(source, x, core)
        side = 0 if step > 0 else 1
        return remote(tile, tile, x_send.at[side, source], x_recv.at[side, source],
                      at.along_x(step))

    def x_half(source, step):
        side = 0 if step > 0 else 1
        rows = pl.ds(0, BLOCK_TOKENS) if step > 0 else pl.ds(BLOCK_TOKENS, TILE_ROWS - BLOCK_TOKENS)
        tile = buf.at[source, at.column(-step), core, rows]
        return remote(tile, tile, h_send.at[side, source], h_recv.at[side, source],
                      at.along_x(step))

    def twin_row(source):
        part = buf.at[source, :, core]
        return remote(part, part, d_send.at[source], d_recv.at[source], at.sibling())

    def both(step, action):
        if step < 1 or step > layers - 1:
            return
        pl.when(z - step >= 0)(lambda: action(z - step, 1))
        pl.when(z + step <= layers - 1)(lambda: action(z + step, -1))

    def arrive(source, way):
        z_arrival(source).wait_recv()
        more = (z < layers - 1) if way > 0 else (z > 0)
        pl.when(more)(lambda: z_next(source, way).start())
        x_copy(source, 1).start()
        x_copy(source, -1).start()

    def across(source, way):
        x_copy(source, 1).wait_recv()
        x_half(source, 1).start()
        x_copy(source, -1).wait_recv()
        x_half(source, -1).start()

    def share_row(source, way):
        x_half(source, 1).wait_recv()
        x_half(source, -1).wait_recv()
        twin_row(source).start()

    for step in range(1, layers + 2):
        both(step, arrive)
        if step == 1:
            for hop in (1, 3, 2):
                row_copy(hop).wait_recv()
                row_from(hop).start()
        both(step - 1, across)
        both(step - 2, share_row)

    twin_copy().wait_recv()
    for hop in (1, 3, 2):
        row_from(hop).wait_recv()
    for step in range(1, layers):
        both(step, lambda source, way: twin_row(source).wait_recv())

    for step in range(1, heads):
        for copy in regroup(step):
            copy.wait_send()
    pl.when(z < layers - 1)(lambda: first_up().wait_send())
    pl.when(z > 0)(lambda: first_down().wait_send())
    twin_copy().wait_send()
    for hop in (1, 3, 2):
        row_copy(hop).wait_send()
        row_from(hop).wait_send()

    def drain(source, way):
        more = (z < layers - 1) if way > 0 else (z > 0)
        pl.when(more)(lambda: z_next(source, way).wait_send())
        for step in (1, -1):
            x_copy(source, step).wait_send()
            x_half(source, step).wait_send()
        twin_row(source).wait_send()

    for step in range(1, layers):
        both(step, drain)


def gather_tiles(keys, values, marks, heads, leaves):
    layers = leaves // ROW
    dma = pltpu.SemaphoreType.DMA
    vmem = pl.BlockSpec(memory_space=pltpu.VMEM)
    return pl.pallas_call(
        functools.partial(gather_kernel, heads, leaves),
        out_shape=(
            jax.ShapeDtypeStruct((2, TILE_ROWS, HEAD_DIM), jnp.bfloat16),
            jax.ShapeDtypeStruct((layers, X_CHIPS, 2, TILE_ROWS, HEAD_DIM), jnp.bfloat16),
        ),
        in_specs=[vmem] * 3,
        out_specs=(vmem, vmem),
        scratch_shapes=[
            dma((2 * heads,)), dma((2 * heads,)),
            dma((layers + 2,)), dma((layers,)),
            dma((X_CHIPS,)), dma((X_CHIPS,)),
            dma((2, layers)), dma((2, layers)),
            dma((2, layers)), dma((2, layers)),
            dma((layers,)), dma((layers,)),
            dma((X_CHIPS,)), dma((X_CHIPS,)),
        ],
        compiler_params=pltpu.CompilerParams(
            collective_id=0, has_side_effects=True, vmem_limit_bytes=VMEM_LIMIT
        ),
        name="gather_tiles",
    )(keys, values, marks)


LANES = 2 * BLOCK_TOKENS
SPAN = CHAIN * BLOCK_TOKENS
PART = 3 * BLOCK_TOKENS
PARTS = SPAN // PART


def attend_kernel(
    table, first, queries, grads, own, buf, dq, selfs, back,
    kcat, vcat, kcat_t, q2, g2, s_scr, l_scr, p_all, d_all,
):
    softmax_scale = HEAD_DIM ** -0.5
    log2_scale = softmax_scale * 1.4426950408889634
    rows = HEADS_PER_GROUP * BLOCK_TOKENS
    nt = (((1,), (1,)), ((), ()))
    back[...] = jnp.zeros_like(back)

    def one_tree(tree, carry):
        kcat[:BLOCK_TOKENS] = own[tree, :BLOCK_TOKENS]
        vcat[:BLOCK_TOKENS] = own[tree, BLOCK_TOKENS:KV_ROWS]
        current = first[tree]
        alive, ranks = [], []
        for link in range(MAX_ANCESTORS):
            active = current >= 0
            rank = jnp.right_shift(jnp.maximum(current, 0), 1)
            place = slice((link + 1) * BLOCK_TOKENS, (link + 2) * BLOCK_TOKENS)

            @pl.when(active)
            def _():
                kcat[place] = buf[rank, :BLOCK_TOKENS]
                vcat[place] = buf[rank, BLOCK_TOKENS:KV_ROWS]

            @pl.when(jnp.logical_not(active))
            def _():
                kcat[place] = own[tree, :BLOCK_TOKENS]
                vcat[place] = own[tree, BLOCK_TOKENS:KV_ROWS]

            alive.append(active)
            ranks.append(rank)
            current = jnp.where(active, table[rank], -1)
        for link in range(CHAIN):
            place = slice(link * BLOCK_TOKENS, (link + 1) * BLOCK_TOKENS)
            kcat_t[:, place] = kcat[place].T
        for head in range(HEADS_PER_GROUP):
            place = slice(head * BLOCK_TOKENS, (head + 1) * BLOCK_TOKENS)
            q2[place] = queries[tree, :, place]
            g2[place] = grads[tree, :, place]

        key_pos = lax.broadcasted_iota(jnp.int32, (BLOCK_TOKENS, LANES), 0)
        row_pos = lax.broadcasted_iota(jnp.int32, (BLOCK_TOKENS, LANES), 1) % BLOCK_TOKENS
        causal = key_pos <= row_pos

        def head_pair(pair, carry):
            lanes = pl.ds(pl.multiple_of(pair * LANES, LANES), LANES)
            q_pair = q2[lanes]
            g_pair = g2[lanes]
            peak = None
            for part in range(PARTS):
                place = slice(part * PART, (part + 1) * PART)
                raw = lax.dot_general(kcat[place], q_pair, nt, preferred_element_type=jnp.float32)
                l_scr[place] = lax.dot_general(
                    vcat[place], g_pair, nt, preferred_element_type=jnp.float32
                )
                for block in range(PART // BLOCK_TOKENS):
                    link = part * (PART // BLOCK_TOKENS) + block
                    score = raw[block * BLOCK_TOKENS:(block + 1) * BLOCK_TOKENS] * log2_scale
                    if link == 0:
                        score = jnp.where(causal, score, masked_score)
                    else:
                        score = score + jnp.where(alive[link - 1], 0.0, masked_score)
                    s_scr[link * BLOCK_TOKENS:(link + 1) * BLOCK_TOKENS] = score
                    top = jnp.max(score.reshape(BLOCK_TOKENS // 8, 8, LANES), 0)
                    peak = top if peak is None else jnp.maximum(peak, top)
            peak = jnp.max(peak, 0, keepdims=True)
            total = jnp.zeros((8, LANES), jnp.float32)
            lean = jnp.zeros((8, LANES), jnp.float32)
            for link in range(CHAIN):
                place = slice(link * BLOCK_TOKENS, (link + 1) * BLOCK_TOKENS)
                shifted = jnp.exp2(s_scr[place] - peak)
                s_scr[place] = shifted
                total = total + jnp.sum(shifted.reshape(-1, 8, LANES), 0)
                lean = lean + jnp.sum((shifted * l_scr[place]).reshape(-1, 8, LANES), 0)
            inverse = 1.0 / jnp.sum(total, 0, keepdims=True)
            mean = jnp.sum(lean, 0, keepdims=True) * inverse
            query_part = jnp.zeros((HEAD_DIM, LANES), jnp.float32)
            for part in range(PARTS):
                place = slice(part * PART, (part + 1) * PART)
                weights = s_scr[place] * inverse
                dscore = (weights * (l_scr[place] - mean)).astype(jnp.bfloat16)
                p_all[place, lanes] = weights.astype(jnp.bfloat16)
                d_all[place, lanes] = dscore
                query_part = query_part + jnp.dot(
                    kcat_t[:, place], dscore, preferred_element_type=jnp.float32
                )
            query_part = (query_part * softmax_scale).T.astype(jnp.bfloat16)
            for half in range(2):
                column = pl.multiple_of(pair * LANES + half * HEAD_DIM, HEAD_DIM)
                dq[tree, :, pl.ds(column, HEAD_DIM)] = query_part[
                    half * BLOCK_TOKENS:(half + 1) * BLOCK_TOKENS
                ]
            return carry

        lax.fori_loop(0, rows // LANES, head_pair, 0)

        for part in range(PARTS):
            place = slice(part * PART, (part + 1) * PART)
            key_part = softmax_scale * jnp.dot(
                d_all[place], q2[...], preferred_element_type=jnp.float32
            )
            value_part = jnp.dot(p_all[place], g2[...], preferred_element_type=jnp.float32)
            for block in range(PART // BLOCK_TOKENS):
                link = part * (PART // BLOCK_TOKENS) + block
                here = slice(block * BLOCK_TOKENS, (block + 1) * BLOCK_TOKENS)
                if link == 0:
                    selfs[tree, :BLOCK_TOKENS] = key_part[here]
                    selfs[tree, BLOCK_TOKENS:] = value_part[here]
                else:

                    @pl.when(alive[link - 1])
                    def _():
                        back[ranks[link - 1], :BLOCK_TOKENS] = key_part[here].astype(jnp.bfloat16)
                        back[ranks[link - 1], BLOCK_TOKENS:] = value_part[here].astype(jnp.bfloat16)

        return carry

    lax.fori_loop(0, 2, one_tree, 0)


def attend(table, first, queries, grads, own, buf):
    leaves = buf.shape[0]
    rows = HEADS_PER_GROUP * BLOCK_TOKENS
    vmem = pl.BlockSpec(memory_space=pltpu.VMEM)
    smem = pl.BlockSpec(memory_space=pltpu.SMEM)
    bf16, f32 = jnp.bfloat16, jnp.float32
    return pl.pallas_call(
        attend_kernel,
        out_shape=(
            jax.ShapeDtypeStruct(queries.shape, bf16),
            jax.ShapeDtypeStruct((2, KV_ROWS, HEAD_DIM), f32),
            jax.ShapeDtypeStruct((leaves, KV_ROWS, HEAD_DIM), bf16),
        ),
        in_specs=[smem, smem, vmem, vmem, vmem, vmem],
        out_specs=(vmem, vmem, vmem),
        scratch_shapes=[
            pltpu.VMEM((SPAN, HEAD_DIM), bf16),
            pltpu.VMEM((SPAN, HEAD_DIM), bf16),
            pltpu.VMEM((HEAD_DIM, SPAN), bf16),
            pltpu.VMEM((rows, HEAD_DIM), bf16),
            pltpu.VMEM((rows, HEAD_DIM), bf16),
            pltpu.VMEM((SPAN, LANES), f32),
            pltpu.VMEM((SPAN, LANES), f32),
            pltpu.VMEM((SPAN, rows), bf16),
            pltpu.VMEM((SPAN, rows), bf16),
        ],
        compiler_params=pltpu.CompilerParams(vmem_limit_bytes=VMEM_LIMIT),
        cost_estimate=pl.CostEstimate(
            flops=10 * SPAN * rows * HEAD_DIM * 2, bytes_accessed=12 << 20,
            transcendentals=2 * SPAN * rows,
        ),
        name="attend",
    )(table, first, queries, grads, own, buf)


def scatter_kernel(
    heads, leaves, selfs, back, key_out, value_out,
    sums, d_in, e_in, x_in, h_in, r_in, z_in, total, final,
    y_send, y_recv, z_send, z_recv, r_send, r_recv, x_send, x_recv, h_send, h_recv,
    d_send, d_recv, e_send, e_recv,
):
    at = Place(heads, leaves)
    layers, z, x, core = at.layers, at.z, at.x, at.core
    share = BLOCK_TOKENS // heads
    f32, bf16 = jnp.float32, jnp.bfloat16
    at.greet()

    def both(step, action):
        if step < 1 or step > layers - 1:
            return
        pl.when(z - step >= 0)(lambda: action(z - step, 1))
        pl.when(z + step <= layers - 1)(lambda: action(z + step, -1))

    def twin_row(source):
        return remote(back.at[source, :, 1 - core], d_in.at[source], d_send.at[source],
                      d_recv.at[source], at.sibling())

    def twin_tile(step):
        column = at.column(step)
        return remote(back.at[z, column, 1 - core], e_in.at[column],
                      e_send.at[step], e_recv.at[step], at.sibling())

    for step in range(layers - 1, 0, -1):
        both(step, lambda source, way: twin_row(source).start())
    for step in range(X_CHIPS):
        twin_tile(step).start()

    keys_half = pl.ds(0, BLOCK_TOKENS)
    values_half = pl.ds(BLOCK_TOKENS, BLOCK_TOKENS)

    def x_half(source, step):
        side = 0 if step > 0 else 1
        rows = values_half if step > 0 else keys_half
        return remote(sums.at[source, at.column(2), rows], h_in.at[side, source],
                      h_send.at[side, source], h_recv.at[side, source], at.along_x(step))

    def x_copy(source, step):
        side = 0 if step > 0 else 1
        return remote(sums.at[source, at.column(step)], x_in.at[side, source],
                      x_send.at[side, source], x_recv.at[side, source], at.along_x(step))

    def z_next(source, way):
        place = source if way > 0 else jnp.where(source == z + 1, layers, source)
        return remote(sums.at[source, x], z_in.at[place], z_send.at[source], z_recv.at[place],
                      at.along_z(-way))

    def z_arrival(place):
        return remote(z_in.at[place], z_in.at[place], z_send.at[z], z_recv.at[place], at.sibling())

    def row_copy(step):
        return remote(sums.at[z, at.column(step)], r_in.at[step], r_send.at[step],
                      r_recv.at[step], at.along_x(step))

    def merge_twin(source, way):
        twin_row(source).wait_recv()
        for column in range(X_CHIPS):
            sums[source, column] = (
                back[source, column, core].astype(f32) + d_in[source, column].astype(f32)
            ).astype(bf16)
        x_half(source, 1).start()
        x_half(source, -1).start()

    def merge_half(source, way):
        x_half(source, 1).wait_recv()
        right = at.column(1)
        sums[source, right, values_half] = (
            sums[source, right, values_half].astype(f32) + h_in[0, source].astype(f32)
        ).astype(bf16)
        x_copy(source, 1).start()
        x_half(source, -1).wait_recv()
        left = at.column(-1)
        sums[source, left, keys_half] = (
            sums[source, left, keys_half].astype(f32) + h_in[1, source].astype(f32)
        ).astype(bf16)
        x_copy(source, -1).start()

    def merge_across(source, way):
        x_copy(source, 1).wait_recv()
        x_copy(source, -1).wait_recv()
        held = (
            sums[source, x].astype(f32)
            + x_in[0, source].astype(f32)
            + x_in[1, source].astype(f32)
        )
        far = (z < layers - 1) if way > 0 else (z > 0)

        @pl.when(far)
        def _():
            z_arrival(source).wait_recv()
            sums[source, x] = (held + z_in[source].astype(f32)).astype(bf16)

        @pl.when(jnp.logical_not(far))
        def _():
            sums[source, x] = held.astype(bf16)

        z_next(source, way).start()

    for step in range(layers - 1, -2, -1):
        both(step, merge_twin)
        if step == 0:
            for hop in (2, 1, 3):
                column = at.column(hop)
                twin_tile(hop).wait_recv()
                sums[z, column] = (
                    back[z, column, core].astype(f32) + e_in[column].astype(f32)
                ).astype(bf16)
                row_copy(hop).start()
        both(step + 1, merge_half)
        both(step + 2, merge_across)

    total[...] = selfs[...]
    twin_tile(0).wait_recv()
    total[core] += e_in[x].astype(f32)
    for hop in (1, 3, 2):
        row_copy(hop).wait_recv()
        tree = (at.column(-hop) < x).astype(jnp.int32)
        total[tree] += r_in[hop].astype(f32)

    @pl.when(z < layers - 1)
    def _():
        z_arrival(z).wait_recv()
        total[0] += z_in[z].astype(f32)

    @pl.when(z > 0)
    def _():
        z_arrival(layers).wait_recv()
        total[1] += z_in[layers].astype(f32)

    final[...] = total[...].astype(bf16)

    def regroup(step):
        peer = (at.y + step) % heads
        column = pl.ds(pl.multiple_of(at.y * HEAD_DIM, HEAD_DIM), HEAD_DIM)
        rows_k = pl.ds(pl.multiple_of(peer * share, share), share)
        rows_v = pl.ds(pl.multiple_of(BLOCK_TOKENS + peer * share, share), share)
        return (
            remote(final.at[:, rows_k, :], key_out.at[:, :, column],
                   y_send.at[2 * step], y_recv.at[2 * step], at.head_peer(step)),
            remote(final.at[:, rows_v, :], value_out.at[:, :, column],
                   y_send.at[2 * step + 1], y_recv.at[2 * step + 1], at.head_peer(step)),
        )

    for step in range(1, heads):
        for copy in regroup(step):
            copy.start()
    mine = pl.ds(pl.multiple_of(at.y * HEAD_DIM, HEAD_DIM), HEAD_DIM)
    key_out[:, :, mine] = final[:, pl.ds(pl.multiple_of(at.y * share, share), share), :]
    value_out[:, :, mine] = final[
        :, pl.ds(pl.multiple_of(BLOCK_TOKENS + at.y * share, share), share), :
    ]
    for step in range(1, heads):
        for copy in regroup(step):
            copy.wait()

    for step in range(X_CHIPS):
        twin_tile(step).wait_send()
    for hop in (1, 3, 2):
        row_copy(hop).wait_send()

    def drain(source, way):
        twin_row(source).wait_send()
        for step in (1, -1):
            x_half(source, step).wait_send()
            x_copy(source, step).wait_send()
        z_next(source, way).wait_send()

    for step in range(1, layers):
        both(step, drain)


def scatter_tiles(selfs, back, heads, leaves):
    layers = leaves // ROW
    dma = pltpu.SemaphoreType.DMA
    vmem = pl.BlockSpec(memory_space=pltpu.VMEM)
    bf16 = jnp.bfloat16
    share = BLOCK_TOKENS // heads
    out = jax.ShapeDtypeStruct((2, share, heads * HEAD_DIM), bf16)
    return pl.pallas_call(
        functools.partial(scatter_kernel, heads, leaves),
        out_shape=(out, out),
        in_specs=[vmem] * 2,
        out_specs=(vmem, vmem),
        scratch_shapes=[
            pltpu.VMEM((layers, X_CHIPS, KV_ROWS, HEAD_DIM), bf16),
            pltpu.VMEM((layers, X_CHIPS, KV_ROWS, HEAD_DIM), bf16),
            pltpu.VMEM((X_CHIPS, KV_ROWS, HEAD_DIM), bf16),
            pltpu.VMEM((2, layers, KV_ROWS, HEAD_DIM), bf16),
            pltpu.VMEM((2, layers, BLOCK_TOKENS, HEAD_DIM), bf16),
            pltpu.VMEM((X_CHIPS, KV_ROWS, HEAD_DIM), bf16),
            pltpu.VMEM((layers + 1, KV_ROWS, HEAD_DIM), bf16),
            pltpu.VMEM((2, KV_ROWS, HEAD_DIM), jnp.float32),
            pltpu.VMEM((2, KV_ROWS, HEAD_DIM), bf16),
            dma((2 * heads,)), dma((2 * heads,)),
            dma((layers,)), dma((layers + 1,)),
            dma((X_CHIPS,)), dma((X_CHIPS,)),
            dma((2, layers)), dma((2, layers)),
            dma((2, layers)), dma((2, layers)),
            dma((layers,)), dma((layers,)),
            dma((X_CHIPS,)), dma((X_CHIPS,)),
        ],
        compiler_params=pltpu.CompilerParams(
            collective_id=1, has_side_effects=True, vmem_limit_bytes=VMEM_LIMIT
        ),
        name="scatter_tiles",
    )(selfs, back)


def body(queries, keys, values, output_gradient, parents):
    heads, leaves = lax.axis_size("head"), lax.axis_size("leaf")
    marks = jnp.broadcast_to(
        parents.astype(jnp.bfloat16)[:, None, None], (2, PARENT_ROWS, HEAD_DIM)
    )
    own, buf = gather_tiles(keys, values, marks, heads, leaves)
    buf = buf.reshape(leaves, TILE_ROWS, HEAD_DIM)
    table = buf[:, KV_ROWS, 0].astype(jnp.int32)
    query_grads, selfs, back = attend(table, parents, queries, output_gradient, own, buf)
    back = back.reshape(leaves // ROW, X_CHIPS, 2, KV_ROWS, HEAD_DIM)
    key_gradient, value_gradient = scatter_tiles(selfs, back, heads, leaves)
    return query_grads, key_gradient, value_gradient


def solution(mesh):
    in_specs = (
        P("leaf", None, "head"),
        P("leaf", "head", None),
        P("leaf", "head", None),
        P("leaf", None, "head"),
        P("leaf"),
    )
    out_specs = (P("leaf", None, "head"), P("leaf", "head", None), P("leaf", "head", None))
    return jax.shard_map(body, mesh=mesh, in_specs=in_specs, out_specs=out_specs, check_vma=False)
```

```python
import functools

import jax
import jax.numpy as jnp
from jax import lax
from jax.experimental import pallas as pl
from jax.experimental.pallas import tpu as pltpu
from jax.sharding import PartitionSpec as P

QUERY_HEAD_COUNT = 64
KEY_VALUE_HEADS = 8
HEAD_DIM = 128
BLOCK_TOKENS = 128
MAX_ANCESTORS = 14
HEADS_PER_GROUP = QUERY_HEAD_COUNT // KEY_VALUE_HEADS
CHAIN = MAX_ANCESTORS + 1

X_CHIPS = 4
ROW = 2 * X_CHIPS
PARENT_ROWS = 16
KV_ROWS = 2 * BLOCK_TOKENS
TILE_ROWS = KV_ROWS + PARENT_ROWS
VMEM_LIMIT = 56 * 1024 * 1024
masked_score = -1e30
MESH = pl.DeviceIdType.MESH


class Place:
    def __init__(self, heads, leaves):
        self.heads, self.layers = heads, leaves // ROW
        self.y = lax.axis_index("head")
        self.leaf = lax.axis_index("leaf")
        self.z = self.leaf // ROW
        self.x = (self.leaf % ROW) // 2
        self.core = self.leaf % 2

    def column(self, step):
        return (self.x + step + X_CHIPS) % X_CHIPS

    def leaf_of(self, z, x, core):
        return z * ROW + x * 2 + core

    def along_x(self, step):
        return (self.y, self.leaf_of(self.z, self.column(step), self.core))

    def along_z(self, step):
        layer = (self.z + step + self.layers) % self.layers
        return (self.y, self.leaf_of(layer, self.x, self.core))

    def sibling(self):
        return (self.y, self.leaf_of(self.z, self.x, 1 - self.core))

    def head_peer(self, step):
        return ((self.y + step) % self.heads, self.leaf)

    def greet(self):
        barrier = pltpu.get_barrier_semaphore()

        def signal(device):
            pl.semaphore_signal(barrier, inc=1, device_id=device, device_id_type=MESH)

        for step in range(1, self.heads):
            signal(self.head_peer(step))
        for step in range(1, X_CHIPS):
            signal(self.along_x(step))
        signal(self.sibling())

        for step in range(1, self.layers):
            signal(self.along_z(step))
        pl.semaphore_wait(barrier, self.heads + self.layers + X_CHIPS - 2)


def remote(src, dst, send_sem, recv_sem, device):
    return pltpu.make_async_remote_copy(
        src_ref=src, dst_ref=dst, send_sem=send_sem, recv_sem=recv_sem,
        device_id=device, device_id_type=MESH,
    )


def gather_kernel(
    heads, leaves, parents, keys, values, own, buf,
    y_send, y_recv, z_send, z_recv, r_send, r_recv, x_send, x_recv, h_send, h_recv,
    d_send, d_recv, e_send, e_recv,
):
    at = Place(heads, leaves)
    layers, z, x, core = at.layers, at.z, at.x, at.core
    share = BLOCK_TOKENS // heads
    at.greet()

    def regroup(step):
        column = pl.ds(pl.multiple_of(((at.y + step) % heads) * HEAD_DIM, HEAD_DIM), HEAD_DIM)
        rows_k = pl.ds(pl.multiple_of(at.y * share, share), share)
        rows_v = pl.ds(pl.multiple_of(BLOCK_TOKENS + at.y * share, share), share)
        peer = at.head_peer(step)
        return (
            remote(keys.at[:, :, column], own.at[:, rows_k, :],
                   y_send.at[2 * step], y_recv.at[2 * step], peer),
            remote(values.at[:, :, column], own.at[:, rows_v, :],
                   y_send.at[2 * step + 1], y_recv.at[2 * step + 1], peer),
        )

    for step in range(1, heads):
        for copy in regroup(step):
            copy.start()
    mine = pl.ds(pl.multiple_of(at.y * HEAD_DIM, HEAD_DIM), HEAD_DIM)
    own[:, pl.ds(pl.multiple_of(at.y * share, share), share), :] = keys[:, :, mine]
    own[:, pl.ds(pl.multiple_of(BLOCK_TOKENS + at.y * share, share), share), :] = values[:, :, mine]
    for tree in range(2):
        own[tree, KV_ROWS:, :] = jnp.full(
            (PARENT_ROWS, HEAD_DIM), parents[tree].astype(jnp.float32), jnp.float32
        ).astype(jnp.bfloat16)
    for step in range(1, heads):
        for copy in regroup(step):
            copy.wait_recv()

    def slot(zz, xx, cc):
        return buf.at[zz, xx, cc]

    def layer_copy(step):
        target = (z + step + layers) % layers
        tree = (target < z).astype(jnp.int32)
        return remote(own.at[tree], slot(z, x, core), z_send.at[step % layers], z_recv.at[z],
                      at.along_z(step))

    nearest_first = []
    for step in range(1, layers // 2 + 1):
        nearest_first += [step] if 2 * step == layers else [step, -step]
    for step in nearest_first:
        layer_copy(step).start()

    def row_copy(step):
        tree = (at.column(step) < x).astype(jnp.int32)
        return remote(own.at[tree], slot(z, x, core), r_send.at[step], r_recv.at[step],
                      at.along_x(step))

    for step in (1, 3, 2):
        row_copy(step).start()

    def twin_copy():
        return remote(own.at[core], slot(z, x, core), e_send.at[0], e_recv.at[0], at.sibling())

    twin_copy().start()

    def row_from(step):
        tile = slot(z, at.column(-step), core)
        return remote(tile, tile, e_send.at[step], e_recv.at[step], at.sibling())

    def z_arrival(source):
        tile = slot(source, x, core)
        return remote(tile, tile, z_send.at[0], z_recv.at[source], at.sibling())

    def x_copy(source, step):
        tile = slot(source, x, core)
        side = 0 if step > 0 else 1
        return remote(tile, tile, x_send.at[side, source], x_recv.at[side, source],
                      at.along_x(step))

    def x_half(source, step):
        side = 0 if step > 0 else 1
        rows = pl.ds(0, BLOCK_TOKENS) if step > 0 else pl.ds(BLOCK_TOKENS, TILE_ROWS - BLOCK_TOKENS)
        tile = buf.at[source, at.column(-step), core, rows]
        return remote(tile, tile, h_send.at[side, source], h_recv.at[side, source],
                      at.along_x(step))

    def twin_row(source):
        part = buf.at[source, :, core]
        return remote(part, part, d_send.at[source], d_recv.at[source], at.sibling())

    def both(step, action):
        if step < 1 or step > layers - 1:
            return
        pl.when(z - step >= 0)(lambda: action(z - step, 1))
        pl.when(z + step <= layers - 1)(lambda: action(z + step, -1))

    def arrive(source, way):
        z_arrival(source).wait_recv()
        x_copy(source, 1).start()
        x_copy(source, -1).start()

    def across(source, way):
        x_copy(source, 1).wait_recv()
        x_half(source, 1).start()
        x_copy(source, -1).wait_recv()
        x_half(source, -1).start()

    def share_row(source, way):
        x_half(source, 1).wait_recv()
        x_half(source, -1).wait_recv()
        twin_row(source).start()

    for step in range(1, layers + 2):
        both(step, arrive)
        if step == 1:
            for hop in (1, 3, 2):
                row_copy(hop).wait_recv()
                row_from(hop).start()
        both(step - 1, across)
        both(step - 2, share_row)

    twin_copy().wait_recv()
    for hop in (1, 3, 2):
        row_from(hop).wait_recv()
    for step in range(1, layers):
        both(step, lambda source, way: twin_row(source).wait_recv())

    for step in range(1, heads):
        for copy in regroup(step):
            copy.wait_send()
    for step in nearest_first:
        layer_copy(step).wait_send()
    twin_copy().wait_send()
    for hop in (1, 3, 2):
        row_copy(hop).wait_send()
        row_from(hop).wait_send()

    def drain(source, way):
        for step in (1, -1):
            x_copy(source, step).wait_send()
            x_half(source, step).wait_send()
        twin_row(source).wait_send()

    for step in range(1, layers):
        both(step, drain)


def gather_tiles(parents, keys, values, heads, leaves):
    layers = leaves // ROW
    dma = pltpu.SemaphoreType.DMA
    vmem = pl.BlockSpec(memory_space=pltpu.VMEM)
    return pl.pallas_call(
        functools.partial(gather_kernel, heads, leaves),
        out_shape=(
            jax.ShapeDtypeStruct((2, TILE_ROWS, HEAD_DIM), jnp.bfloat16),
            jax.ShapeDtypeStruct((layers, X_CHIPS, 2, TILE_ROWS, HEAD_DIM), jnp.bfloat16),
        ),
        in_specs=[pl.BlockSpec(memory_space=pltpu.SMEM), vmem, vmem],
        out_specs=(vmem, vmem),
        scratch_shapes=[
            dma((2 * heads,)), dma((2 * heads,)),
            dma((layers,)), dma((layers,)),
            dma((X_CHIPS,)), dma((X_CHIPS,)),
            dma((2, layers)), dma((2, layers)),
            dma((2, layers)), dma((2, layers)),
            dma((layers,)), dma((layers,)),
            dma((X_CHIPS,)), dma((X_CHIPS,)),
        ],
        compiler_params=pltpu.CompilerParams(
            collective_id=0, has_side_effects=True, vmem_limit_bytes=VMEM_LIMIT
        ),
        name="gather_tiles",
    )(parents, keys, values)


LANES = 2 * BLOCK_TOKENS
SPAN = CHAIN * BLOCK_TOKENS
PART = 3 * BLOCK_TOKENS
PARTS = SPAN // PART


def attend_kernel(
    first, queries, grads, own, buf, dq, selfs, back,
    kcat, vcat, kcat_t, q2, g2, s_scr, l_scr, p_all, d_all, links, table, table_sem,
):
    softmax_scale = HEAD_DIM ** -0.5
    log2_scale = softmax_scale * 1.4426950408889634
    rows = HEADS_PER_GROUP * BLOCK_TOKENS
    nt = (((1,), (1,)), ((), ()))
    leaves = buf.shape[0]
    marks = buf[:, KV_ROWS:KV_ROWS + 8, :][:, 0, :].astype(jnp.float32)
    marks = jnp.concatenate([marks, jnp.zeros((HEAD_DIM - leaves, HEAD_DIM), jnp.float32)]).T
    links[...] = marks[:8].astype(jnp.int32)
    to_scalars = pltpu.make_async_copy(links, table, table_sem)
    to_scalars.start()
    back[...] = jnp.zeros_like(back)
    to_scalars.wait()

    def one_tree(tree, carry):
        kcat[:BLOCK_TOKENS] = own[tree, :BLOCK_TOKENS]
        vcat[:BLOCK_TOKENS] = own[tree, BLOCK_TOKENS:KV_ROWS]
        current = first[tree]
        alive, ranks = [], []
        for link in range(MAX_ANCESTORS):
            active = current >= 0
            rank = jnp.right_shift(jnp.maximum(current, 0), 1)
            place = slice((link + 1) * BLOCK_TOKENS, (link + 2) * BLOCK_TOKENS)

            @pl.when(active)
            def _():
                kcat[place] = buf[rank, :BLOCK_TOKENS]
                vcat[place] = buf[rank, BLOCK_TOKENS:KV_ROWS]

            @pl.when(jnp.logical_not(active))
            def _():
                kcat[place] = own[tree, :BLOCK_TOKENS]
                vcat[place] = own[tree, BLOCK_TOKENS:KV_ROWS]

            alive.append(active)
            ranks.append(rank)
            current = jnp.where(active, table[0, rank], -1)
        for link in range(CHAIN):
            place = slice(link * BLOCK_TOKENS, (link + 1) * BLOCK_TOKENS)
            kcat_t[:, place] = kcat[place].T
        for head in range(HEADS_PER_GROUP):
            place = slice(head * BLOCK_TOKENS, (head + 1) * BLOCK_TOKENS)
            q2[place] = queries[tree, :, place]
            g2[place] = grads[tree, :, place]

        key_pos = lax.broadcasted_iota(jnp.int32, (BLOCK_TOKENS, LANES), 0)
        row_pos = lax.broadcasted_iota(jnp.int32, (BLOCK_TOKENS, LANES), 1) % BLOCK_TOKENS
        causal = key_pos <= row_pos

        bias = [jnp.float32(0.0)] + [jnp.where(on, 0.0, masked_score) for on in alive]

        def lanes_of(pair):
            return slice(pair * LANES, (pair + 1) * LANES)

        def place_of(link):
            return slice(link * BLOCK_TOKENS, (link + 1) * BLOCK_TOKENS)

        def score_block(pair, link, peak):
            place, lanes, turn = place_of(link), lanes_of(pair), pair % 2
            raw = lax.dot_general(kcat[place], q2[lanes], nt, preferred_element_type=jnp.float32)
            if link == 0:
                raw = jnp.where(causal, raw, masked_score)
            s_scr[turn, place] = raw
            l_scr[turn, place] = lax.dot_general(
                vcat[place], g2[lanes], nt, preferred_element_type=jnp.float32
            )
            top = jnp.max(raw.reshape(-1, 8, LANES), 0) * log2_scale + bias[link]
            return top if peak is None else jnp.maximum(peak, top)

        def sum_block(pair, link, peak, total, lean):
            turn = pair % 2
            offset = jnp.broadcast_to(bias[link] - peak, (16, LANES))
            for row in range(link * BLOCK_TOKENS, (link + 1) * BLOCK_TOKENS, 16):
                slab = slice(row, row + 16)
                shifted = jnp.exp2(s_scr[turn, slab] * log2_scale + offset)
                s_scr[turn, slab] = shifted
                total = total + shifted
                lean = lean + shifted * l_scr[turn, slab]
            return total, lean

        def weight_block(pair, link, inverse, mean):
            lanes, turn = lanes_of(pair), pair % 2
            for row in range(link * BLOCK_TOKENS, (link + 1) * BLOCK_TOKENS, 16):
                slab = slice(row, row + 16)
                weights = s_scr[turn, slab] * inverse
                d_all[slab, lanes] = (weights * (l_scr[turn, slab] - mean)).astype(jnp.bfloat16)
                p_all[slab, lanes] = weights.astype(jnp.bfloat16)

        def query_part(pair):
            part = jnp.dot(
                kcat_t[...], d_all[:, lanes_of(pair)], preferred_element_type=jnp.float32
            )
            part = (part * softmax_scale).T.astype(jnp.bfloat16)
            for half in range(2):
                head = 2 * pair + half
                dq[tree, :, place_of(head)] = part[place_of(half)]

        pairs = rows // LANES
        peak = None
        for link in range(CHAIN):
            peak = score_block(0, link, peak)
        for pair in range(pairs):
            peak = jnp.max(peak, 0, keepdims=True)
            total = jnp.zeros((16, LANES), jnp.float32)
            lean = jnp.zeros((16, LANES), jnp.float32)
            later = None
            half = (CHAIN + 1) // 2
            for link in range(CHAIN):
                total, lean = sum_block(pair, link, peak, total, lean)
                if pair + 1 < pairs and link % 2 == 0:
                    later = score_block(pair + 1, link // 2, later)
            inverse = 1.0 / jnp.sum(total, 0, keepdims=True)
            mean = jnp.sum(lean, 0, keepdims=True) * inverse
            for link in range(CHAIN):
                weight_block(pair, link, inverse, mean)
                if pair + 1 < pairs and link % 2 == 1:
                    later = score_block(pair + 1, half + link // 2, later)
            query_part(pair)
            peak = later

        for part in range(PARTS):
            place = slice(part * PART, (part + 1) * PART)
            key_part = softmax_scale * jnp.dot(
                d_all[place], q2[...], preferred_element_type=jnp.float32
            )
            value_part = jnp.dot(p_all[place], g2[...], preferred_element_type=jnp.float32)
            for block in range(PART // BLOCK_TOKENS):
                link = part * (PART // BLOCK_TOKENS) + block
                here = slice(block * BLOCK_TOKENS, (block + 1) * BLOCK_TOKENS)
                if link == 0:
                    selfs[tree, :BLOCK_TOKENS] = key_part[here]
                    selfs[tree, BLOCK_TOKENS:] = value_part[here]
                else:

                    @pl.when(alive[link - 1])
                    def _():
                        back[ranks[link - 1], :BLOCK_TOKENS] = key_part[here].astype(jnp.bfloat16)
                        back[ranks[link - 1], BLOCK_TOKENS:] = value_part[here].astype(jnp.bfloat16)

        return carry

    lax.fori_loop(0, 2, one_tree, 0)


def attend(first, queries, grads, own, buf):
    leaves = buf.shape[0]
    rows = HEADS_PER_GROUP * BLOCK_TOKENS
    vmem = pl.BlockSpec(memory_space=pltpu.VMEM)
    smem = pl.BlockSpec(memory_space=pltpu.SMEM)
    bf16, f32 = jnp.bfloat16, jnp.float32
    return pl.pallas_call(
        attend_kernel,
        out_shape=(
            jax.ShapeDtypeStruct(queries.shape, bf16),
            jax.ShapeDtypeStruct((2, KV_ROWS, HEAD_DIM), f32),
            jax.ShapeDtypeStruct((leaves, KV_ROWS, HEAD_DIM), bf16),
        ),
        in_specs=[smem, vmem, vmem, vmem, vmem],
        out_specs=(vmem, vmem, vmem),
        scratch_shapes=[
            pltpu.VMEM((SPAN, HEAD_DIM), bf16),
            pltpu.VMEM((SPAN, HEAD_DIM), bf16),
            pltpu.VMEM((HEAD_DIM, SPAN), bf16),
            pltpu.VMEM((rows, HEAD_DIM), bf16),
            pltpu.VMEM((rows, HEAD_DIM), bf16),
            pltpu.VMEM((2, SPAN, LANES), f32),
            pltpu.VMEM((2, SPAN, LANES), f32),
            pltpu.VMEM((SPAN, rows), bf16),
            pltpu.VMEM((SPAN, rows), bf16),
            pltpu.VMEM((8, HEAD_DIM), jnp.int32),
            pltpu.SMEM((8, HEAD_DIM), jnp.int32),
            pltpu.SemaphoreType.DMA,
        ],
        compiler_params=pltpu.CompilerParams(vmem_limit_bytes=VMEM_LIMIT),
        cost_estimate=pl.CostEstimate(
            flops=10 * SPAN * rows * HEAD_DIM * 2, bytes_accessed=12 << 20,
            transcendentals=2 * SPAN * rows,
        ),
        name="attend",
    )(first, queries, grads, own, buf)


def scatter_kernel(
    heads, leaves, selfs, back, key_out, value_out,
    sums, d_in, e_in, x_in, h_in, r_in, z_in, total, final,
    y_send, y_recv, z_send, z_recv, r_send, r_recv, x_send, x_recv, h_send, h_recv,
    d_send, d_recv, e_send, e_recv,
):
    at = Place(heads, leaves)
    layers, z, x, core = at.layers, at.z, at.x, at.core
    share = BLOCK_TOKENS // heads
    f32, bf16 = jnp.float32, jnp.bfloat16
    at.greet()

    def both(step, action):
        if step < 1 or step > layers - 1:
            return
        pl.when(z - step >= 0)(lambda: action(z - step, 1))
        pl.when(z + step <= layers - 1)(lambda: action(z + step, -1))

    def twin_row(source):
        return remote(back.at[source, :, 1 - core], d_in.at[source], d_send.at[source],
                      d_recv.at[source], at.sibling())

    def twin_tile(step):
        column = at.column(step)
        return remote(back.at[z, column, 1 - core], e_in.at[column],
                      e_send.at[step], e_recv.at[step], at.sibling())

    for step in range(layers - 1, 0, -1):
        both(step, lambda source, way: twin_row(source).start())
    for step in range(X_CHIPS):
        twin_tile(step).start()

    keys_half = pl.ds(0, BLOCK_TOKENS)
    values_half = pl.ds(BLOCK_TOKENS, BLOCK_TOKENS)

    def x_half(source, step):
        side = 0 if step > 0 else 1
        rows = values_half if step > 0 else keys_half
        return remote(sums.at[source, at.column(2), rows], h_in.at[side, source],
                      h_send.at[side, source], h_recv.at[side, source], at.along_x(step))

    def x_copy(source, step):
        side = 0 if step > 0 else 1
        return remote(sums.at[source, at.column(step)], x_in.at[side, source],
                      x_send.at[side, source], x_recv.at[side, source], at.along_x(step))

    def z_home(source, way):
        return remote(sums.at[source, x], z_in.at[z], z_send.at[source], z_recv.at[z],
                      (at.y, at.leaf_of(source, x, core)))

    def z_arrival(source):
        return remote(z_in.at[source], z_in.at[source], z_send.at[z], z_recv.at[source],
                      at.sibling())

    def row_copy(step):
        return remote(sums.at[z, at.column(step)], r_in.at[step], r_send.at[step],
                      r_recv.at[step], at.along_x(step))

    def merge_twin(source, way):
        twin_row(source).wait_recv()
        for column in range(X_CHIPS):
            sums[source, column] = (
                back[source, column, core].astype(f32) + d_in[source, column].astype(f32)
            ).astype(bf16)
        x_half(source, 1).start()
        x_half(source, -1).start()

    def merge_half(source, way):
        x_half(source, 1).wait_recv()
        right = at.column(1)
        sums[source, right, values_half] = (
            sums[source, right, values_half].astype(f32) + h_in[0, source].astype(f32)
        ).astype(bf16)
        x_copy(source, 1).start()
        x_half(source, -1).wait_recv()
        left = at.column(-1)
        sums[source, left, keys_half] = (
            sums[source, left, keys_half].astype(f32) + h_in[1, source].astype(f32)
        ).astype(bf16)
        x_copy(source, -1).start()

    def merge_across(source, way):
        x_copy(source, 1).wait_recv()
        x_copy(source, -1).wait_recv()
        sums[source, x] = (
            sums[source, x].astype(f32)
            + x_in[0, source].astype(f32)
            + x_in[1, source].astype(f32)
        ).astype(bf16)
        z_home(source, way).start()

    for step in range(layers - 1, -2, -1):
        both(step, merge_twin)
        if step == 0:
            for hop in (2, 1, 3):
                column = at.column(hop)
                twin_tile(hop).wait_recv()
                sums[z, column] = (
                    back[z, column, core].astype(f32) + e_in[column].astype(f32)
                ).astype(bf16)
                row_copy(hop).start()
        both(step + 1, merge_half)
        both(step + 2, merge_across)

    total[...] = selfs[...]
    twin_tile(0).wait_recv()
    total[core] += e_in[x].astype(f32)
    for hop in (1, 3, 2):
        row_copy(hop).wait_recv()
        tree = (at.column(-hop) < x).astype(jnp.int32)
        total[tree] += r_in[hop].astype(f32)

    def take(source, way):
        z_arrival(source).wait_recv()
        tree = (source < z).astype(jnp.int32)
        total[tree] += z_in[source].astype(f32)

    for step in range(layers - 1, 0, -1):
        both(step, take)

    final[...] = total[...].astype(bf16)

    def regroup(step):
        peer = (at.y + step) % heads
        column = pl.ds(pl.multiple_of(at.y * HEAD_DIM, HEAD_DIM), HEAD_DIM)
        rows_k = pl.ds(pl.multiple_of(peer * share, share), share)
        rows_v = pl.ds(pl.multiple_of(BLOCK_TOKENS + peer * share, share), share)
        return (
            remote(final.at[:, rows_k, :], key_out.at[:, :, column],
                   y_send.at[2 * step], y_recv.at[2 * step], at.head_peer(step)),
            remote(final.at[:, rows_v, :], value_out.at[:, :, column],
                   y_send.at[2 * step + 1], y_recv.at[2 * step + 1], at.head_peer(step)),
        )

    for step in range(1, heads):
        for copy in regroup(step):
            copy.start()
    mine = pl.ds(pl.multiple_of(at.y * HEAD_DIM, HEAD_DIM), HEAD_DIM)
    key_out[:, :, mine] = final[:, pl.ds(pl.multiple_of(at.y * share, share), share), :]
    value_out[:, :, mine] = final[
        :, pl.ds(pl.multiple_of(BLOCK_TOKENS + at.y * share, share), share), :
    ]
    for step in range(1, heads):
        for copy in regroup(step):
            copy.wait()

    for step in range(X_CHIPS):
        twin_tile(step).wait_send()
    for hop in (1, 3, 2):
        row_copy(hop).wait_send()

    def drain(source, way):
        twin_row(source).wait_send()
        for step in (1, -1):
            x_half(source, step).wait_send()
            x_copy(source, step).wait_send()
        z_home(source, way).wait_send()

    for step in range(1, layers):
        both(step, drain)


def scatter_tiles(selfs, back, heads, leaves):
    layers = leaves // ROW
    dma = pltpu.SemaphoreType.DMA
    vmem = pl.BlockSpec(memory_space=pltpu.VMEM)
    bf16 = jnp.bfloat16
    share = BLOCK_TOKENS // heads
    out = jax.ShapeDtypeStruct((2, share, heads * HEAD_DIM), bf16)
    return pl.pallas_call(
        functools.partial(scatter_kernel, heads, leaves),
        out_shape=(out, out),
        in_specs=[vmem] * 2,
        out_specs=(vmem, vmem),
        scratch_shapes=[
            pltpu.VMEM((layers, X_CHIPS, KV_ROWS, HEAD_DIM), bf16),
            pltpu.VMEM((layers, X_CHIPS, KV_ROWS, HEAD_DIM), bf16),
            pltpu.VMEM((X_CHIPS, KV_ROWS, HEAD_DIM), bf16),
            pltpu.VMEM((2, layers, KV_ROWS, HEAD_DIM), bf16),
            pltpu.VMEM((2, layers, BLOCK_TOKENS, HEAD_DIM), bf16),
            pltpu.VMEM((X_CHIPS, KV_ROWS, HEAD_DIM), bf16),
            pltpu.VMEM((layers, KV_ROWS, HEAD_DIM), bf16),
            pltpu.VMEM((2, KV_ROWS, HEAD_DIM), jnp.float32),
            pltpu.VMEM((2, KV_ROWS, HEAD_DIM), bf16),
            dma((2 * heads,)), dma((2 * heads,)),
            dma((layers,)), dma((layers,)),
            dma((X_CHIPS,)), dma((X_CHIPS,)),
            dma((2, layers)), dma((2, layers)),
            dma((2, layers)), dma((2, layers)),
            dma((layers,)), dma((layers,)),
            dma((X_CHIPS,)), dma((X_CHIPS,)),
        ],
        compiler_params=pltpu.CompilerParams(
            collective_id=1, has_side_effects=True, vmem_limit_bytes=VMEM_LIMIT
        ),
        name="scatter_tiles",
    )(selfs, back)


def body(queries, keys, values, output_gradient, parents):
    heads, leaves = lax.axis_size("head"), lax.axis_size("leaf")
    own, buf = gather_tiles(parents, keys, values, heads, leaves)
    buf = buf.reshape(leaves, TILE_ROWS, HEAD_DIM)
    query_grads, selfs, back = attend(parents, queries, output_gradient, own, buf)
    back = back.reshape(leaves // ROW, X_CHIPS, 2, KV_ROWS, HEAD_DIM)
    key_gradient, value_gradient = scatter_tiles(selfs, back, heads, leaves)
    return query_grads, key_gradient, value_gradient


def solution(mesh):
    in_specs = (
        P("leaf", None, "head"),
        P("leaf", "head", None),
        P("leaf", "head", None),
        P("leaf", None, "head"),
        P("leaf"),
    )
    out_specs = (P("leaf", None, "head"), P("leaf", "head", None), P("leaf", "head", None))
    return jax.shard_map(body, mesh=mesh, in_specs=in_specs, out_specs=out_specs, check_vma=False)
```

```python
import functools

import jax
import jax.numpy as jnp
from jax import lax
from jax.experimental import pallas as pl
from jax.experimental.pallas import tpu as pltpu
from jax.sharding import PartitionSpec as P

QUERY_HEAD_COUNT = 64
KEY_VALUE_HEADS = 8
HEAD_DIM = 128
BLOCK_TOKENS = 128
MAX_ANCESTORS = 14
HEADS_PER_GROUP = QUERY_HEAD_COUNT // KEY_VALUE_HEADS
CHAIN = MAX_ANCESTORS + 1

X_CHIPS = 4
ROW = 2 * X_CHIPS
PARENT_ROWS = 16
KV_ROWS = 2 * BLOCK_TOKENS
TILE_ROWS = KV_ROWS + PARENT_ROWS
GATHER_VMEM = 10 * 1024 * 1024
ATTEND_VMEM = 30 * 1024 * 1024
SCATTER_VMEM = 18 * 1024 * 1024
masked_score = -1e30
MESH = pl.DeviceIdType.MESH


class Place:
    def __init__(self, heads, leaves):
        self.heads, self.layers = heads, leaves // ROW
        self.y = lax.axis_index("head")
        self.leaf = lax.axis_index("leaf")
        self.z = self.leaf // ROW
        self.x = (self.leaf % ROW) // 2
        self.core = self.leaf % 2

    def column(self, step):
        return (self.x + step + X_CHIPS) % X_CHIPS

    def leaf_of(self, z, x, core):
        return z * ROW + x * 2 + core

    def along_x(self, step):
        return (self.y, self.leaf_of(self.z, self.column(step), self.core))

    def along_z(self, step):
        layer = (self.z + step + self.layers) % self.layers
        return (self.y, self.leaf_of(layer, self.x, self.core))

    def sibling(self):
        return (self.y, self.leaf_of(self.z, self.x, 1 - self.core))

    def head_peer(self, step):
        return ((self.y + step) % self.heads, self.leaf)

    def layers_at(self, distance):
        if distance < 1 or 2 * distance > self.layers:
            return []
        below = (self.z - distance + self.layers) % self.layers
        above = (self.z + distance) % self.layers
        return [below] if 2 * distance == self.layers else [below, above]

    def greet(self):
        barrier = pltpu.get_barrier_semaphore()

        def signal(device):
            pl.semaphore_signal(barrier, inc=1, device_id=device, device_id_type=MESH)

        for step in range(1, self.heads):
            signal(self.head_peer(step))
        for step in range(1, X_CHIPS):
            signal(self.along_x(step))
        signal(self.sibling())

        for step in range(1, self.layers):
            signal(self.along_z(step))
        pl.semaphore_wait(barrier, self.heads + self.layers + X_CHIPS - 2)


def remote(src, dst, send_sem, recv_sem, device):
    return pltpu.make_async_remote_copy(
        src_ref=src, dst_ref=dst, send_sem=send_sem, recv_sem=recv_sem,
        device_id=device, device_id_type=MESH,
    )


def gather_kernel(
    heads, leaves, parents, keys, values, own, buf,
    y_send, y_recv, z_send, z_recv, r_send, r_recv, x_send, x_recv, h_send, h_recv,
    d_send, d_recv, e_send, e_recv,
):
    at = Place(heads, leaves)
    layers, z, x, core = at.layers, at.z, at.x, at.core
    share = BLOCK_TOKENS // heads
    at.greet()

    def regroup(step):
        column = pl.ds(pl.multiple_of(((at.y + step) % heads) * HEAD_DIM, HEAD_DIM), HEAD_DIM)
        rows_k = pl.ds(pl.multiple_of(at.y * share, share), share)
        rows_v = pl.ds(pl.multiple_of(BLOCK_TOKENS + at.y * share, share), share)
        peer = at.head_peer(step)
        return (
            remote(keys.at[:, :, column], own.at[:, rows_k, :],
                   y_send.at[2 * step], y_recv.at[2 * step], peer),
            remote(values.at[:, :, column], own.at[:, rows_v, :],
                   y_send.at[2 * step + 1], y_recv.at[2 * step + 1], peer),
        )

    for step in range(1, heads):
        for copy in regroup(step):
            copy.start()
    mine = pl.ds(pl.multiple_of(at.y * HEAD_DIM, HEAD_DIM), HEAD_DIM)
    own[:, pl.ds(pl.multiple_of(at.y * share, share), share), :] = keys[:, :, mine]
    own[:, pl.ds(pl.multiple_of(BLOCK_TOKENS + at.y * share, share), share), :] = values[:, :, mine]
    for tree in range(2):
        own[tree, KV_ROWS:, :] = jnp.full(
            (PARENT_ROWS, HEAD_DIM), parents[tree].astype(jnp.float32), jnp.float32
        ).astype(jnp.bfloat16)
    for step in range(1, heads):
        for copy in regroup(step):
            copy.wait_recv()

    def slot(zz, xx, cc):
        return buf.at[zz, xx, cc]

    def layer_copy(step):
        target = (z + step + layers) % layers
        tree = (target < z).astype(jnp.int32)
        return remote(own.at[tree], slot(z, x, core), z_send.at[step % layers], z_recv.at[z],
                      at.along_z(step))

    nearest_first = []
    for step in range(1, layers // 2 + 1):
        nearest_first += [step] if 2 * step == layers else [step, -step]
    for step in nearest_first:
        layer_copy(step).start()

    def row_copy(step):
        tree = (at.column(step) < x).astype(jnp.int32)
        return remote(own.at[tree], slot(z, x, core), r_send.at[step], r_recv.at[step],
                      at.along_x(step))

    for step in (1, 3, 2):
        row_copy(step).start()

    def twin_copy():
        return remote(own.at[core], slot(z, x, core), e_send.at[0], e_recv.at[0], at.sibling())

    twin_copy().start()

    def row_from(step):
        tile = slot(z, at.column(-step), core)
        return remote(tile, tile, e_send.at[step], e_recv.at[step], at.sibling())

    def z_arrival(source):
        tile = slot(source, x, core)
        return remote(tile, tile, z_send.at[0], z_recv.at[source], at.sibling())

    def x_copy(source, step):
        tile = slot(source, x, core)
        side = 0 if step > 0 else 1
        return remote(tile, tile, x_send.at[side, source], x_recv.at[side, source],
                      at.along_x(step))

    def x_half(source, step):
        side = 0 if step > 0 else 1
        rows = pl.ds(0, BLOCK_TOKENS) if step > 0 else pl.ds(BLOCK_TOKENS, TILE_ROWS - BLOCK_TOKENS)
        tile = buf.at[source, at.column(-step), core, rows]
        return remote(tile, tile, h_send.at[side, source], h_recv.at[side, source],
                      at.along_x(step))

    def twin_row(source):
        part = buf.at[source, :, core]
        return remote(part, part, d_send.at[source], d_recv.at[source], at.sibling())

    def each(distance, action):
        for source in at.layers_at(distance):
            action(source)

    def arrive(source):
        z_arrival(source).wait_recv()
        x_copy(source, 1).start()
        x_copy(source, -1).start()

    def across(source):
        x_copy(source, 1).wait_recv()
        x_half(source, 1).start()
        x_copy(source, -1).wait_recv()
        x_half(source, -1).start()

    def share_row(source):
        x_half(source, 1).wait_recv()
        x_half(source, -1).wait_recv()
        twin_row(source).start()

    reach = layers // 2
    for step in range(1, reach + 3):
        each(step, arrive)
        if step == 1:
            for hop in (1, 3, 2):
                row_copy(hop).wait_recv()
                row_from(hop).start()
        each(step - 1, across)
        each(step - 2, share_row)

    twin_copy().wait_recv()
    for hop in (1, 3, 2):
        row_from(hop).wait_recv()
    for step in range(1, reach + 1):
        each(step, lambda source: twin_row(source).wait_recv())

    for step in range(1, heads):
        for copy in regroup(step):
            copy.wait_send()
    for step in nearest_first:
        layer_copy(step).wait_send()
    twin_copy().wait_send()
    for hop in (1, 3, 2):
        row_copy(hop).wait_send()
        row_from(hop).wait_send()

    def drain(source):
        for step in (1, -1):
            x_copy(source, step).wait_send()
            x_half(source, step).wait_send()
        twin_row(source).wait_send()

    for step in range(1, layers // 2 + 1):
        each(step, drain)


def gather_tiles(parents, keys, values, heads, leaves):
    layers = leaves // ROW
    dma = pltpu.SemaphoreType.DMA
    vmem = pl.BlockSpec(memory_space=pltpu.VMEM)
    return pl.pallas_call(
        functools.partial(gather_kernel, heads, leaves),
        out_shape=(
            jax.ShapeDtypeStruct((2, TILE_ROWS, HEAD_DIM), jnp.bfloat16),
            jax.ShapeDtypeStruct((layers, X_CHIPS, 2, TILE_ROWS, HEAD_DIM), jnp.bfloat16),
        ),
        in_specs=[pl.BlockSpec(memory_space=pltpu.SMEM), vmem, vmem],
        out_specs=(vmem, vmem),
        scratch_shapes=[
            dma((2 * heads,)), dma((2 * heads,)),
            dma((layers,)), dma((layers,)),
            dma((X_CHIPS,)), dma((X_CHIPS,)),
            dma((2, layers)), dma((2, layers)),
            dma((2, layers)), dma((2, layers)),
            dma((layers,)), dma((layers,)),
            dma((X_CHIPS,)), dma((X_CHIPS,)),
        ],
        compiler_params=pltpu.CompilerParams(
            collective_id=0, has_side_effects=True, vmem_limit_bytes=GATHER_VMEM
        ),
        cost_estimate=pl.CostEstimate(
            flops=1 << 34, bytes_accessed=8 << 20, transcendentals=0
        ),
        name="gather_tiles",
    )(parents, keys, values)


LANES = 2 * BLOCK_TOKENS
SPAN = CHAIN * BLOCK_TOKENS
PART = 3 * BLOCK_TOKENS
PARTS = SPAN // PART


def attend_kernel(
    first, queries, grads, own, buf, dq, selfs, back,
    kcat, vcat, kcat_t, q2, g2, s_scr, l_scr, p_all, d_all, links, table, table_sem,
):
    softmax_scale = HEAD_DIM ** -0.5
    log2_scale = softmax_scale * 1.4426950408889634
    rows = HEADS_PER_GROUP * BLOCK_TOKENS
    nt = (((1,), (1,)), ((), ()))
    leaves = buf.shape[0]
    marks = buf[:, KV_ROWS:KV_ROWS + 8, :][:, 0, :].astype(jnp.float32)
    marks = jnp.concatenate([marks, jnp.zeros((HEAD_DIM - leaves, HEAD_DIM), jnp.float32)]).T
    links[...] = marks[:8].astype(jnp.int32)
    to_scalars = pltpu.make_async_copy(links, table, table_sem)
    to_scalars.start()
    back[...] = jnp.zeros_like(back)
    to_scalars.wait()

    def one_tree(tree, carry):
        kcat[:BLOCK_TOKENS] = own[tree, :BLOCK_TOKENS]
        vcat[:BLOCK_TOKENS] = own[tree, BLOCK_TOKENS:KV_ROWS]
        current = first[tree]
        alive, ranks = [], []
        for link in range(MAX_ANCESTORS):
            active = current >= 0
            rank = jnp.right_shift(jnp.maximum(current, 0), 1)
            place = slice((link + 1) * BLOCK_TOKENS, (link + 2) * BLOCK_TOKENS)

            @pl.when(active)
            def _():
                kcat[place] = buf[rank, :BLOCK_TOKENS]
                vcat[place] = buf[rank, BLOCK_TOKENS:KV_ROWS]

            @pl.when(jnp.logical_not(active))
            def _():
                kcat[place] = own[tree, :BLOCK_TOKENS]
                vcat[place] = own[tree, BLOCK_TOKENS:KV_ROWS]

            alive.append(active)
            ranks.append(rank)
            current = jnp.where(active, table[0, rank], -1)
        for link in range(CHAIN):
            place = slice(link * BLOCK_TOKENS, (link + 1) * BLOCK_TOKENS)
            kcat_t[:, place] = kcat[place].T
        for head in range(HEADS_PER_GROUP):
            place = slice(head * BLOCK_TOKENS, (head + 1) * BLOCK_TOKENS)
            q2[place] = queries[tree, :, place]
            g2[place] = grads[tree, :, place]

        key_pos = lax.broadcasted_iota(jnp.int32, (BLOCK_TOKENS, LANES), 0)
        row_pos = lax.broadcasted_iota(jnp.int32, (BLOCK_TOKENS, LANES), 1) % BLOCK_TOKENS
        causal = key_pos <= row_pos

        bias = [jnp.float32(0.0)] + [jnp.where(on, 0.0, masked_score) for on in alive]

        def lanes_of(pair):
            return slice(pair * LANES, (pair + 1) * LANES)

        def place_of(link):
            return slice(link * BLOCK_TOKENS, (link + 1) * BLOCK_TOKENS)

        def score_block(pair, link, peak):
            place, lanes, turn = place_of(link), lanes_of(pair), pair % 2
            raw = lax.dot_general(kcat[place], q2[lanes], nt, preferred_element_type=jnp.float32)
            if link == 0:
                raw = jnp.where(causal, raw, masked_score)
            s_scr[turn, place] = raw
            l_scr[turn, place] = lax.dot_general(
                vcat[place], g2[lanes], nt, preferred_element_type=jnp.float32
            )
            top = jnp.max(raw.reshape(-1, 8, LANES), 0) * log2_scale + bias[link]
            return top if peak is None else jnp.maximum(peak, top)

        def sum_block(pair, link, peak, total, lean):
            turn = pair % 2
            offset = jnp.broadcast_to(bias[link] - peak, (16, LANES))
            for row in range(link * BLOCK_TOKENS, (link + 1) * BLOCK_TOKENS, 16):
                slab = slice(row, row + 16)
                shifted = jnp.exp2(s_scr[turn, slab] * log2_scale + offset)
                s_scr[turn, slab] = shifted
                total = total + shifted
                lean = lean + shifted * l_scr[turn, slab]
            return total, lean

        def weight_block(pair, link, inverse, mean):
            lanes, turn = lanes_of(pair), pair % 2
            for row in range(link * BLOCK_TOKENS, (link + 1) * BLOCK_TOKENS, 16):
                slab = slice(row, row + 16)
                weights = s_scr[turn, slab] * inverse
                d_all[slab, lanes] = (weights * (l_scr[turn, slab] - mean)).astype(jnp.bfloat16)
                p_all[slab, lanes] = weights.astype(jnp.bfloat16)

        def query_part(pair):
            part = jnp.dot(
                kcat_t[...], d_all[:, lanes_of(pair)], preferred_element_type=jnp.float32
            )
            part = (part * softmax_scale).T.astype(jnp.bfloat16)
            for half in range(2):
                head = 2 * pair + half
                dq[tree, :, place_of(head)] = part[place_of(half)]

        pairs = rows // LANES
        peak = None
        for link in range(CHAIN):
            peak = score_block(0, link, peak)
        for pair in range(pairs):
            peak = jnp.max(peak, 0, keepdims=True)
            total = jnp.zeros((16, LANES), jnp.float32)
            lean = jnp.zeros((16, LANES), jnp.float32)
            later = None
            half = (CHAIN + 1) // 2
            for link in range(CHAIN):
                total, lean = sum_block(pair, link, peak, total, lean)
                if pair + 1 < pairs and link % 2 == 0:
                    later = score_block(pair + 1, link // 2, later)
            inverse = 1.0 / jnp.sum(total, 0, keepdims=True)
            mean = jnp.sum(lean, 0, keepdims=True) * inverse
            for link in range(CHAIN):
                weight_block(pair, link, inverse, mean)
                if pair + 1 < pairs and link % 2 == 1:
                    later = score_block(pair + 1, half + link // 2, later)
            query_part(pair)
            peak = later

        for part in range(PARTS):
            place = slice(part * PART, (part + 1) * PART)
            key_part = softmax_scale * jnp.dot(
                d_all[place], q2[...], preferred_element_type=jnp.float32
            )
            value_part = jnp.dot(p_all[place], g2[...], preferred_element_type=jnp.float32)
            for block in range(PART // BLOCK_TOKENS):
                link = part * (PART // BLOCK_TOKENS) + block
                here = slice(block * BLOCK_TOKENS, (block + 1) * BLOCK_TOKENS)
                if link == 0:
                    selfs[tree, :BLOCK_TOKENS] = key_part[here]
                    selfs[tree, BLOCK_TOKENS:] = value_part[here]
                else:

                    @pl.when(alive[link - 1])
                    def _():
                        back[ranks[link - 1], :BLOCK_TOKENS] = key_part[here].astype(jnp.bfloat16)
                        back[ranks[link - 1], BLOCK_TOKENS:] = value_part[here].astype(jnp.bfloat16)

        return carry

    lax.fori_loop(0, 2, one_tree, 0)


def attend(first, queries, grads, own, buf):
    leaves = buf.shape[0]
    rows = HEADS_PER_GROUP * BLOCK_TOKENS
    vmem = pl.BlockSpec(memory_space=pltpu.VMEM)
    smem = pl.BlockSpec(memory_space=pltpu.SMEM)
    bf16, f32 = jnp.bfloat16, jnp.float32
    return pl.pallas_call(
        attend_kernel,
        out_shape=(
            jax.ShapeDtypeStruct(queries.shape, bf16),
            jax.ShapeDtypeStruct((2, KV_ROWS, HEAD_DIM), f32),
            jax.ShapeDtypeStruct((leaves, KV_ROWS, HEAD_DIM), bf16),
        ),
        in_specs=[smem, vmem, vmem, vmem, vmem],
        out_specs=(vmem, vmem, vmem),
        scratch_shapes=[
            pltpu.VMEM((SPAN, HEAD_DIM), bf16),
            pltpu.VMEM((SPAN, HEAD_DIM), bf16),
            pltpu.VMEM((HEAD_DIM, SPAN), bf16),
            pltpu.VMEM((rows, HEAD_DIM), bf16),
            pltpu.VMEM((rows, HEAD_DIM), bf16),
            pltpu.VMEM((2, SPAN, LANES), f32),
            pltpu.VMEM((2, SPAN, LANES), f32),
            pltpu.VMEM((SPAN, rows), bf16),
            pltpu.VMEM((SPAN, rows), bf16),
            pltpu.VMEM((8, HEAD_DIM), jnp.int32),
            pltpu.SMEM((8, HEAD_DIM), jnp.int32),
            pltpu.SemaphoreType.DMA,
        ],
        compiler_params=pltpu.CompilerParams(vmem_limit_bytes=ATTEND_VMEM),
        cost_estimate=pl.CostEstimate(
            flops=10 * SPAN * rows * HEAD_DIM * 2, bytes_accessed=12 << 20,
            transcendentals=2 * SPAN * rows,
        ),
        name="attend",
    )(first, queries, grads, own, buf)


def scatter_kernel(
    heads, leaves, selfs, back, key_out, value_out,
    sums, d_in, e_in, x_in, h_in, r_in, z_in, total, final,
    y_send, y_recv, z_send, z_recv, r_send, r_recv, x_send, x_recv, h_send, h_recv,
    d_send, d_recv, e_send, e_recv,
):
    at = Place(heads, leaves)
    layers, z, x, core = at.layers, at.z, at.x, at.core
    share = BLOCK_TOKENS // heads
    f32, bf16 = jnp.float32, jnp.bfloat16
    at.greet()

    def each(distance, action):
        for source in at.layers_at(distance):
            action(source)

    def twin_row(source):
        return remote(back.at[source, :, 1 - core], d_in.at[source], d_send.at[source],
                      d_recv.at[source], at.sibling())

    def twin_tile(step):
        column = at.column(step)
        return remote(back.at[z, column, 1 - core], e_in.at[column],
                      e_send.at[step], e_recv.at[step], at.sibling())

    reach = layers // 2
    for step in range(reach, 0, -1):
        each(step, lambda source: twin_row(source).start())
    for step in range(X_CHIPS):
        twin_tile(step).start()

    keys_half = pl.ds(0, BLOCK_TOKENS)
    values_half = pl.ds(BLOCK_TOKENS, BLOCK_TOKENS)

    def x_half(source, step):
        side = 0 if step > 0 else 1
        rows = values_half if step > 0 else keys_half
        return remote(sums.at[source, at.column(2), rows], h_in.at[side, source],
                      h_send.at[side, source], h_recv.at[side, source], at.along_x(step))

    def x_copy(source, step):
        side = 0 if step > 0 else 1
        return remote(sums.at[source, at.column(step)], x_in.at[side, source],
                      x_send.at[side, source], x_recv.at[side, source], at.along_x(step))

    def z_home(source):
        return remote(sums.at[source, x], z_in.at[z], z_send.at[source], z_recv.at[z],
                      (at.y, at.leaf_of(source, x, core)))

    def z_arrival(source):
        return remote(z_in.at[source], z_in.at[source], z_send.at[z], z_recv.at[source],
                      at.sibling())

    def row_copy(step):
        return remote(sums.at[z, at.column(step)], r_in.at[step], r_send.at[step],
                      r_recv.at[step], at.along_x(step))

    def merge_twin(source):
        twin_row(source).wait_recv()
        for column in range(X_CHIPS):
            sums[source, column] = (
                back[source, column, core].astype(f32) + d_in[source, column].astype(f32)
            ).astype(bf16)
        x_half(source, 1).start()
        x_half(source, -1).start()

    def merge_half(source):
        x_half(source, 1).wait_recv()
        right = at.column(1)
        sums[source, right, values_half] = (
            sums[source, right, values_half].astype(f32) + h_in[0, source].astype(f32)
        ).astype(bf16)
        x_copy(source, 1).start()
        x_half(source, -1).wait_recv()
        left = at.column(-1)
        sums[source, left, keys_half] = (
            sums[source, left, keys_half].astype(f32) + h_in[1, source].astype(f32)
        ).astype(bf16)
        x_copy(source, -1).start()

    def merge_across(source):
        x_copy(source, 1).wait_recv()
        x_copy(source, -1).wait_recv()
        sums[source, x] = (
            sums[source, x].astype(f32)
            + x_in[0, source].astype(f32)
            + x_in[1, source].astype(f32)
        ).astype(bf16)
        z_home(source).start()

    for step in range(reach, -2, -1):
        each(step, merge_twin)
        if step == 0:
            for hop in (2, 1, 3):
                column = at.column(hop)
                twin_tile(hop).wait_recv()
                sums[z, column] = (
                    back[z, column, core].astype(f32) + e_in[column].astype(f32)
                ).astype(bf16)
                row_copy(hop).start()
        each(step + 1, merge_half)
        each(step + 2, merge_across)

    total[...] = selfs[...]
    twin_tile(0).wait_recv()
    total[core] += e_in[x].astype(f32)
    for hop in (1, 3, 2):
        row_copy(hop).wait_recv()
        tree = (at.column(-hop) < x).astype(jnp.int32)
        total[tree] += r_in[hop].astype(f32)

    def take(source):
        z_arrival(source).wait_recv()
        tree = (source < z).astype(jnp.int32)
        total[tree] += z_in[source].astype(f32)

    for step in range(reach, 0, -1):
        each(step, take)

    final[...] = total[...].astype(bf16)

    def regroup(step):
        peer = (at.y + step) % heads
        column = pl.ds(pl.multiple_of(at.y * HEAD_DIM, HEAD_DIM), HEAD_DIM)
        rows_k = pl.ds(pl.multiple_of(peer * share, share), share)
        rows_v = pl.ds(pl.multiple_of(BLOCK_TOKENS + peer * share, share), share)
        return (
            remote(final.at[:, rows_k, :], key_out.at[:, :, column],
                   y_send.at[2 * step], y_recv.at[2 * step], at.head_peer(step)),
            remote(final.at[:, rows_v, :], value_out.at[:, :, column],
                   y_send.at[2 * step + 1], y_recv.at[2 * step + 1], at.head_peer(step)),
        )

    for step in range(1, heads):
        for copy in regroup(step):
            copy.start()
    mine = pl.ds(pl.multiple_of(at.y * HEAD_DIM, HEAD_DIM), HEAD_DIM)
    key_out[:, :, mine] = final[:, pl.ds(pl.multiple_of(at.y * share, share), share), :]
    value_out[:, :, mine] = final[
        :, pl.ds(pl.multiple_of(BLOCK_TOKENS + at.y * share, share), share), :
    ]
    for step in range(1, heads):
        for copy in regroup(step):
            copy.wait()

    for step in range(X_CHIPS):
        twin_tile(step).wait_send()
    for hop in (1, 3, 2):
        row_copy(hop).wait_send()

    def drain(source):
        twin_row(source).wait_send()
        for step in (1, -1):
            x_half(source, step).wait_send()
            x_copy(source, step).wait_send()
        z_home(source).wait_send()

    for step in range(1, layers // 2 + 1):
        each(step, drain)


def scatter_tiles(selfs, back, heads, leaves):
    layers = leaves // ROW
    dma = pltpu.SemaphoreType.DMA
    vmem = pl.BlockSpec(memory_space=pltpu.VMEM)
    bf16 = jnp.bfloat16
    share = BLOCK_TOKENS // heads
    out = jax.ShapeDtypeStruct((2, share, heads * HEAD_DIM), bf16)
    return pl.pallas_call(
        functools.partial(scatter_kernel, heads, leaves),
        out_shape=(out, out),
        in_specs=[vmem] * 2,
        out_specs=(vmem, vmem),
        scratch_shapes=[
            pltpu.VMEM((layers, X_CHIPS, KV_ROWS, HEAD_DIM), bf16),
            pltpu.VMEM((layers, X_CHIPS, KV_ROWS, HEAD_DIM), bf16),
            pltpu.VMEM((X_CHIPS, KV_ROWS, HEAD_DIM), bf16),
            pltpu.VMEM((2, layers, KV_ROWS, HEAD_DIM), bf16),
            pltpu.VMEM((2, layers, BLOCK_TOKENS, HEAD_DIM), bf16),
            pltpu.VMEM((X_CHIPS, KV_ROWS, HEAD_DIM), bf16),
            pltpu.VMEM((layers, KV_ROWS, HEAD_DIM), bf16),
            pltpu.VMEM((2, KV_ROWS, HEAD_DIM), jnp.float32),
            pltpu.VMEM((2, KV_ROWS, HEAD_DIM), bf16),
            dma((2 * heads,)), dma((2 * heads,)),
            dma((layers,)), dma((layers,)),
            dma((X_CHIPS,)), dma((X_CHIPS,)),
            dma((2, layers)), dma((2, layers)),
            dma((2, layers)), dma((2, layers)),
            dma((layers,)), dma((layers,)),
            dma((X_CHIPS,)), dma((X_CHIPS,)),
        ],
        compiler_params=pltpu.CompilerParams(
            collective_id=1, has_side_effects=True, vmem_limit_bytes=SCATTER_VMEM
        ),
        cost_estimate=pl.CostEstimate(
            flops=1 << 34, bytes_accessed=8 << 20, transcendentals=0
        ),
        name="scatter_tiles",
    )(selfs, back)


def body(queries, keys, values, output_gradient, parents):
    heads, leaves = lax.axis_size("head"), lax.axis_size("leaf")
    own, buf = gather_tiles(parents, keys, values, heads, leaves)
    buf = buf.reshape(leaves, TILE_ROWS, HEAD_DIM)
    query_grads, selfs, back = attend(parents, queries, output_gradient, own, buf)
    back = back.reshape(leaves // ROW, X_CHIPS, 2, KV_ROWS, HEAD_DIM)
    key_gradient, value_gradient = scatter_tiles(selfs, back, heads, leaves)
    return query_grads, key_gradient, value_gradient


def solution(mesh):
    in_specs = (
        P("leaf", None, "head"),
        P("leaf", "head", None),
        P("leaf", "head", None),
        P("leaf", None, "head"),
        P("leaf"),
    )
    out_specs = (P("leaf", None, "head"), P("leaf", "head", None), P("leaf", "head", None))
    return jax.shard_map(body, mesh=mesh, in_specs=in_specs, out_specs=out_specs, check_vma=False)
```

```python
import functools

import jax
import jax.numpy as jnp
from jax import lax
from jax.experimental import pallas as pl
from jax.experimental.pallas import tpu as pltpu
from jax.sharding import PartitionSpec as P

QUERY_HEAD_COUNT = 64
KEY_VALUE_HEADS = 8
HEAD_DIM = 128
BLOCK_TOKENS = 128
MAX_ANCESTORS = 14
HEADS_PER_GROUP = QUERY_HEAD_COUNT // KEY_VALUE_HEADS
CHAIN = MAX_ANCESTORS + 1

X_CHIPS = 4
ROW = 2 * X_CHIPS
PARENT_ROWS = 8
KV_ROWS = 2 * BLOCK_TOKENS
TILE_ROWS = KV_ROWS + PARENT_ROWS
GATHER_VMEM = 10 * 1024 * 1024
ATTEND_VMEM = 30 * 1024 * 1024
SCATTER_VMEM = 18 * 1024 * 1024
masked_score = -1e30
MESH = pl.DeviceIdType.MESH


class Place:
    def __init__(self, heads, leaves):
        self.heads, self.layers = heads, leaves // ROW
        self.y = lax.axis_index("head")
        self.leaf = lax.axis_index("leaf")
        self.z = self.leaf // ROW
        self.x = (self.leaf % ROW) // 2
        self.core = self.leaf % 2

    def column(self, step):
        return (self.x + step + X_CHIPS) % X_CHIPS

    def leaf_of(self, z, x, core):
        return z * ROW + x * 2 + core

    def along_x(self, step):
        return (self.y, self.leaf_of(self.z, self.column(step), self.core))

    def along_z(self, step):
        layer = (self.z + step + self.layers) % self.layers
        return (self.y, self.leaf_of(layer, self.x, self.core))

    def sibling(self):
        return (self.y, self.leaf_of(self.z, self.x, 1 - self.core))

    def head_peer(self, step):
        return ((self.y + step) % self.heads, self.leaf)

    def layers_at(self, distance):
        if distance < 1 or 2 * distance > self.layers:
            return []
        below = (self.z - distance + self.layers) % self.layers
        above = (self.z + distance) % self.layers
        return [below] if 2 * distance == self.layers else [below, above]

    def greet(self):
        barrier = pltpu.get_barrier_semaphore()

        def signal(device):
            pl.semaphore_signal(barrier, inc=1, device_id=device, device_id_type=MESH)

        for step in range(1, self.heads):
            signal(self.head_peer(step))
        for step in range(1, X_CHIPS):
            signal(self.along_x(step))
        signal(self.sibling())

        for step in range(1, self.layers):
            signal(self.along_z(step))
        pl.semaphore_wait(barrier, self.heads + self.layers + X_CHIPS - 2)


def remote(src, dst, send_sem, recv_sem, device):
    return pltpu.make_async_remote_copy(
        src_ref=src, dst_ref=dst, send_sem=send_sem, recv_sem=recv_sem,
        device_id=device, device_id_type=MESH,
    )


def gather_kernel(
    heads, leaves, parents, local, own, buf,
    y_send, y_recv, z_send, z_recv, r_send, r_recv, x_send, x_recv, h_send, h_recv,
    d_send, d_recv, e_send, e_recv,
):
    at = Place(heads, leaves)
    layers, z, x, core = at.layers, at.z, at.x, at.core
    share = BLOCK_TOKENS // heads
    at.greet()

    def regroup(step):
        column = pl.ds(pl.multiple_of(((at.y + step) % heads) * HEAD_DIM, HEAD_DIM), HEAD_DIM)
        rows_k = pl.ds(pl.multiple_of(at.y * share, share), share)
        rows_v = pl.ds(pl.multiple_of(BLOCK_TOKENS + at.y * share, share), share)
        peer = at.head_peer(step)
        return (
            remote(local.at[:, pl.ds(0, share), column], own.at[:, rows_k, :],
                   y_send.at[2 * step], y_recv.at[2 * step], peer),
            remote(local.at[:, pl.ds(share, share), column], own.at[:, rows_v, :],
                   y_send.at[2 * step + 1], y_recv.at[2 * step + 1], peer),
        )

    for step in range(1, heads):
        for copy in regroup(step):
            copy.start()
    mine = pl.ds(pl.multiple_of(at.y * HEAD_DIM, HEAD_DIM), HEAD_DIM)
    own[:, pl.ds(pl.multiple_of(at.y * share, share), share), :] = local[:, :share, mine]
    own[:, pl.ds(pl.multiple_of(BLOCK_TOKENS + at.y * share, share), share), :] = local[
        :, share:2 * share, mine
    ]
    for tree in range(2):
        own[tree, KV_ROWS:, :] = jnp.full(
            (PARENT_ROWS, HEAD_DIM), parents[tree].astype(jnp.float32), jnp.float32
        ).astype(jnp.bfloat16)
    for step in range(1, heads):
        for copy in regroup(step):
            copy.wait_recv()

    def slot(zz, xx, cc):
        return buf.at[zz, xx, cc]

    def layer_copy(step):
        target = (z + step + layers) % layers
        tree = (target < z).astype(jnp.int32)
        return remote(own.at[tree], slot(z, x, core), z_send.at[step % layers], z_recv.at[z],
                      at.along_z(step))

    nearest_first = []
    for step in range(1, layers // 2 + 1):
        nearest_first += [step] if 2 * step == layers else [step, -step]
    for step in nearest_first:
        layer_copy(step).start()

    def row_copy(step):
        tree = (at.column(step) < x).astype(jnp.int32)
        return remote(own.at[tree], slot(z, x, core), r_send.at[step], r_recv.at[step],
                      at.along_x(step))

    for step in (1, 3, 2):
        row_copy(step).start()

    def twin_copy():
        return remote(own.at[core], slot(z, x, core), e_send.at[0], e_recv.at[0], at.sibling())

    twin_copy().start()

    def row_from(step):
        tile = slot(z, at.column(-step), core)
        return remote(tile, tile, e_send.at[step], e_recv.at[step], at.sibling())

    def z_arrival(source):
        tile = slot(source, x, core)
        return remote(tile, tile, z_send.at[0], z_recv.at[source], at.sibling())

    def x_copy(source, step):
        tile = slot(source, x, core)
        side = 0 if step > 0 else 1
        return remote(tile, tile, x_send.at[side, source], x_recv.at[side, source],
                      at.along_x(step))

    def x_half(source, step):
        side = 0 if step > 0 else 1
        rows = pl.ds(0, BLOCK_TOKENS) if step > 0 else pl.ds(BLOCK_TOKENS, TILE_ROWS - BLOCK_TOKENS)
        tile = buf.at[source, at.column(-step), core, rows]
        return remote(tile, tile, h_send.at[side, source], h_recv.at[side, source],
                      at.along_x(step))

    def twin_row(source):
        part = buf.at[source, :, core]
        return remote(part, part, d_send.at[source], d_recv.at[source], at.sibling())

    def each(distance, action):
        for source in at.layers_at(distance):
            action(source)

    def arrive(source):
        z_arrival(source).wait_recv()
        x_copy(source, 1).start()
        x_copy(source, -1).start()

    def across(source):
        x_copy(source, 1).wait_recv()
        x_half(source, 1).start()
        x_copy(source, -1).wait_recv()
        x_half(source, -1).start()

    def share_row(source):
        x_half(source, 1).wait_recv()
        x_half(source, -1).wait_recv()
        twin_row(source).start()

    reach = layers // 2
    for step in range(1, reach + 3):
        each(step, arrive)
        if step == 1:
            for hop in (1, 3, 2):
                row_copy(hop).wait_recv()
                row_from(hop).start()
        each(step - 1, across)
        each(step - 2, share_row)

    twin_copy().wait_recv()
    for hop in (1, 3, 2):
        row_from(hop).wait_recv()
    for step in range(1, reach + 1):
        each(step, lambda source: twin_row(source).wait_recv())

    for step in range(1, heads):
        for copy in regroup(step):
            copy.wait_send()
    for step in nearest_first:
        layer_copy(step).wait_send()
    twin_copy().wait_send()
    for hop in (1, 3, 2):
        row_copy(hop).wait_send()
        row_from(hop).wait_send()

    def drain(source):
        for step in (1, -1):
            x_copy(source, step).wait_send()
            x_half(source, step).wait_send()
        twin_row(source).wait_send()

    for step in range(1, layers // 2 + 1):
        each(step, drain)


def gather_tiles(parents, local, heads, leaves):
    layers = leaves // ROW
    dma = pltpu.SemaphoreType.DMA
    vmem = pl.BlockSpec(memory_space=pltpu.VMEM)
    return pl.pallas_call(
        functools.partial(gather_kernel, heads, leaves),
        out_shape=(
            jax.ShapeDtypeStruct((2, TILE_ROWS, HEAD_DIM), jnp.bfloat16),
            jax.ShapeDtypeStruct((layers, X_CHIPS, 2, TILE_ROWS, HEAD_DIM), jnp.bfloat16),
        ),
        in_specs=[pl.BlockSpec(memory_space=pltpu.SMEM), vmem],
        out_specs=(vmem, vmem),
        scratch_shapes=[
            dma((2 * heads,)), dma((2 * heads,)),
            dma((layers,)), dma((layers,)),
            dma((X_CHIPS,)), dma((X_CHIPS,)),
            dma((2, layers)), dma((2, layers)),
            dma((2, layers)), dma((2, layers)),
            dma((layers,)), dma((layers,)),
            dma((X_CHIPS,)), dma((X_CHIPS,)),
        ],
        compiler_params=pltpu.CompilerParams(
            collective_id=0, has_side_effects=True, vmem_limit_bytes=GATHER_VMEM
        ),
        cost_estimate=pl.CostEstimate(
            flops=1 << 34, bytes_accessed=8 << 20, transcendentals=0
        ),
        name="gather_tiles",
    )(parents, local)


LANES = 2 * BLOCK_TOKENS
SPAN = CHAIN * BLOCK_TOKENS
PART = CHAIN * BLOCK_TOKENS
PARTS = SPAN // PART
GROUP = 5


def attend_kernel(
    first, queries, grads, own, buf, dq, selfs, back,
    kcat, vcat, kcat_t, q2, g2, s_scr, l_scr, p_all, d_all, links, table, table_sem,
):
    softmax_scale = HEAD_DIM ** -0.5
    log2_scale = softmax_scale * 1.4426950408889634
    rows = HEADS_PER_GROUP * BLOCK_TOKENS
    nt = (((1,), (1,)), ((), ()))
    leaves = buf.shape[0]
    marks = buf[:, KV_ROWS:KV_ROWS + 8, :][:, 0, :].astype(jnp.float32)
    marks = jnp.concatenate([marks, jnp.zeros((HEAD_DIM - leaves, HEAD_DIM), jnp.float32)]).T
    links[...] = marks[:8].astype(jnp.int32)
    to_scalars = pltpu.make_async_copy(links, table, table_sem)
    to_scalars.start()
    back[...] = jnp.zeros_like(back)
    to_scalars.wait()

    def one_tree(tree, carry):
        kcat[:BLOCK_TOKENS] = own[tree, :BLOCK_TOKENS]
        vcat[:BLOCK_TOKENS] = own[tree, BLOCK_TOKENS:KV_ROWS]
        current = first[tree]
        alive, ranks = [], []
        for link in range(MAX_ANCESTORS):
            active = current >= 0
            rank = jnp.right_shift(jnp.maximum(current, 0), 1)
            place = slice((link + 1) * BLOCK_TOKENS, (link + 2) * BLOCK_TOKENS)

            @pl.when(active)
            def _():
                kcat[place] = buf[rank, :BLOCK_TOKENS]
                vcat[place] = buf[rank, BLOCK_TOKENS:KV_ROWS]

            @pl.when(jnp.logical_not(active))
            def _():
                kcat[place] = own[tree, :BLOCK_TOKENS]
                vcat[place] = own[tree, BLOCK_TOKENS:KV_ROWS]

            alive.append(active)
            ranks.append(rank)
            current = jnp.where(active, table[0, rank], -1)
        for link in range(CHAIN):
            place = slice(link * BLOCK_TOKENS, (link + 1) * BLOCK_TOKENS)
            kcat_t[:, place] = kcat[place].T
        for head in range(HEADS_PER_GROUP):
            place = slice(head * BLOCK_TOKENS, (head + 1) * BLOCK_TOKENS)
            q2[place] = queries[tree, :, place]
            g2[place] = grads[tree, :, place]

        key_pos = lax.broadcasted_iota(jnp.int32, (BLOCK_TOKENS, LANES), 0)
        row_pos = lax.broadcasted_iota(jnp.int32, (BLOCK_TOKENS, LANES), 1) % BLOCK_TOKENS
        causal = key_pos <= row_pos

        bias = [jnp.float32(0.0)] + [jnp.where(on, 0.0, masked_score) for on in alive]

        def lanes_of(pair):
            return slice(pair * LANES, (pair + 1) * LANES)

        def place_of(link):
            return slice(link * BLOCK_TOKENS, (link + 1) * BLOCK_TOKENS)

        def score_group(pair, group, peak):
            lanes, turn = lanes_of(pair), pair % 2
            place = slice(group * GROUP * BLOCK_TOKENS, (group + 1) * GROUP * BLOCK_TOKENS)
            s_scr[turn, place] = lax.dot_general(
                kcat[place], q2[lanes], nt, preferred_element_type=jnp.float32
            )
            l_scr[turn, place] = lax.dot_general(
                vcat[place], g2[lanes], nt, preferred_element_type=jnp.float32
            )
            for link in range(group * GROUP, (group + 1) * GROUP):
                here = place_of(link)
                if link == 0:
                    s_scr[turn, here] = jnp.where(causal, s_scr[turn, here], masked_score)
                top = s_scr[turn, here.start:here.start + 16]
                for row in range(here.start + 16, here.stop, 16):
                    top = jnp.maximum(top, s_scr[turn, row:row + 16])
                top = top * log2_scale + bias[link]
                peak = top if peak is None else jnp.maximum(peak, top)
            return peak

        def sum_block(pair, link, peak, total, lean):
            turn = pair % 2
            offset = jnp.broadcast_to(bias[link] - peak, (16, LANES))
            for row in range(link * BLOCK_TOKENS, (link + 1) * BLOCK_TOKENS, 16):
                slab = slice(row, row + 16)
                shifted = jnp.exp2(s_scr[turn, slab] * log2_scale + offset)
                s_scr[turn, slab] = shifted
                total = total + shifted
                lean = lean + shifted * l_scr[turn, slab]
            return total, lean

        def weight_block(pair, link, inverse, mean):
            lanes, turn = lanes_of(pair), pair % 2
            for row in range(link * BLOCK_TOKENS, (link + 1) * BLOCK_TOKENS, 16):
                slab = slice(row, row + 16)
                weights = s_scr[turn, slab] * inverse
                d_all[slab, lanes] = (weights * (l_scr[turn, slab] - mean)).astype(jnp.bfloat16)
                p_all[slab, lanes] = weights.astype(jnp.bfloat16)

        def query_part(pair):
            part = jnp.dot(
                kcat_t[...], d_all[:, lanes_of(pair)], preferred_element_type=jnp.float32
            )
            part = (part * softmax_scale).T.astype(jnp.bfloat16)
            for half in range(2):
                head = 2 * pair + half
                dq[tree, :, place_of(head)] = part[place_of(half)]

        pairs = rows // LANES
        peak = None
        groups = CHAIN // GROUP
        for group in range(groups):
            peak = score_group(0, group, peak)
        for pair in range(pairs):
            peak = jnp.max(peak, 0, keepdims=True)
            total = jnp.zeros((16, LANES), jnp.float32)
            lean = jnp.zeros((16, LANES), jnp.float32)
            later = None
            done = 0
            for link in range(CHAIN):
                total, lean = sum_block(pair, link, peak, total, lean)
                if pair + 1 < pairs and done < groups and 2 * done * CHAIN <= link * 2 * groups:
                    later = score_group(pair + 1, done, later)
                    done += 1
            inverse = 1.0 / jnp.sum(total, 0, keepdims=True)
            mean = jnp.sum(lean, 0, keepdims=True) * inverse
            for link in range(CHAIN):
                weight_block(pair, link, inverse, mean)
            query_part(pair)
            peak = later

        for part in range(PARTS):
            place = slice(part * PART, (part + 1) * PART)
            key_part = softmax_scale * jnp.dot(
                d_all[place], q2[...], preferred_element_type=jnp.float32
            )
            value_part = jnp.dot(p_all[place], g2[...], preferred_element_type=jnp.float32)
            for block in range(PART // BLOCK_TOKENS):
                link = part * (PART // BLOCK_TOKENS) + block
                here = slice(block * BLOCK_TOKENS, (block + 1) * BLOCK_TOKENS)
                if link == 0:
                    selfs[tree, :BLOCK_TOKENS] = key_part[here]
                    selfs[tree, BLOCK_TOKENS:] = value_part[here]
                else:

                    @pl.when(alive[link - 1])
                    def _():
                        back[ranks[link - 1], :BLOCK_TOKENS] = key_part[here].astype(jnp.bfloat16)
                        back[ranks[link - 1], BLOCK_TOKENS:] = value_part[here].astype(jnp.bfloat16)

        return carry

    lax.fori_loop(0, 2, one_tree, 0)


def attend(first, queries, grads, own, buf):
    leaves = buf.shape[0]
    rows = HEADS_PER_GROUP * BLOCK_TOKENS
    vmem = pl.BlockSpec(memory_space=pltpu.VMEM)
    smem = pl.BlockSpec(memory_space=pltpu.SMEM)
    bf16, f32 = jnp.bfloat16, jnp.float32
    return pl.pallas_call(
        attend_kernel,
        out_shape=(
            jax.ShapeDtypeStruct(queries.shape, bf16),
            jax.ShapeDtypeStruct((2, KV_ROWS, HEAD_DIM), f32),
            jax.ShapeDtypeStruct((leaves, KV_ROWS, HEAD_DIM), bf16),
        ),
        in_specs=[smem, vmem, vmem, vmem, vmem],
        out_specs=(vmem, vmem, vmem),
        scratch_shapes=[
            pltpu.VMEM((SPAN, HEAD_DIM), bf16),
            pltpu.VMEM((SPAN, HEAD_DIM), bf16),
            pltpu.VMEM((HEAD_DIM, SPAN), bf16),
            pltpu.VMEM((rows, HEAD_DIM), bf16),
            pltpu.VMEM((rows, HEAD_DIM), bf16),
            pltpu.VMEM((2, SPAN, LANES), f32),
            pltpu.VMEM((2, SPAN, LANES), f32),
            pltpu.VMEM((SPAN, rows), bf16),
            pltpu.VMEM((SPAN, rows), bf16),
            pltpu.VMEM((8, HEAD_DIM), jnp.int32),
            pltpu.SMEM((8, HEAD_DIM), jnp.int32),
            pltpu.SemaphoreType.DMA,
        ],
        compiler_params=pltpu.CompilerParams(vmem_limit_bytes=ATTEND_VMEM),
        cost_estimate=pl.CostEstimate(
            flops=10 * SPAN * rows * HEAD_DIM * 2, bytes_accessed=12 << 20,
            transcendentals=2 * SPAN * rows,
        ),
        name="attend",
    )(first, queries, grads, own, buf)


def scatter_kernel(
    heads, leaves, selfs, back, key_out, value_out,
    sums, d_in, e_in, x_in, h_in, r_in, z_in, total, final,
    y_send, y_recv, z_send, z_recv, r_send, r_recv, x_send, x_recv, h_send, h_recv,
    d_send, d_recv, e_send, e_recv,
):
    at = Place(heads, leaves)
    layers, z, x, core = at.layers, at.z, at.x, at.core
    share = BLOCK_TOKENS // heads
    f32, bf16 = jnp.float32, jnp.bfloat16
    at.greet()

    def each(distance, action):
        for source in at.layers_at(distance):
            action(source)

    def twin_row(source):
        return remote(back.at[source, :, 1 - core], d_in.at[source], d_send.at[source],
                      d_recv.at[source], at.sibling())

    def twin_tile(step):
        column = at.column(step)
        return remote(back.at[z, column, 1 - core], e_in.at[column],
                      e_send.at[step], e_recv.at[step], at.sibling())

    reach = layers // 2
    for step in range(reach, 0, -1):
        each(step, lambda source: twin_row(source).start())
    for step in range(X_CHIPS):
        twin_tile(step).start()

    keys_half = pl.ds(0, BLOCK_TOKENS)
    values_half = pl.ds(BLOCK_TOKENS, BLOCK_TOKENS)

    def x_half(source, step):
        side = 0 if step > 0 else 1
        rows = values_half if step > 0 else keys_half
        return remote(sums.at[source, at.column(2), rows], h_in.at[side, source],
                      h_send.at[side, source], h_recv.at[side, source], at.along_x(step))

    def x_copy(source, step):
        side = 0 if step > 0 else 1
        return remote(sums.at[source, at.column(step)], x_in.at[side, source],
                      x_send.at[side, source], x_recv.at[side, source], at.along_x(step))

    def z_home(source):
        return remote(sums.at[source, x], z_in.at[z], z_send.at[source], z_recv.at[z],
                      (at.y, at.leaf_of(source, x, core)))

    def z_arrival(source):
        return remote(z_in.at[source], z_in.at[source], z_send.at[z], z_recv.at[source],
                      at.sibling())

    def row_copy(step):
        return remote(sums.at[z, at.column(step)], r_in.at[step], r_send.at[step],
                      r_recv.at[step], at.along_x(step))

    def merge_twin(source):
        twin_row(source).wait_recv()
        for column in range(X_CHIPS):
            sums[source, column] = (
                back[source, column, core].astype(f32) + d_in[source, column].astype(f32)
            ).astype(bf16)
        x_half(source, 1).start()
        x_half(source, -1).start()

    def merge_half(source):
        x_half(source, 1).wait_recv()
        right = at.column(1)
        sums[source, right, values_half] = (
            sums[source, right, values_half].astype(f32) + h_in[0, source].astype(f32)
        ).astype(bf16)
        x_copy(source, 1).start()
        x_half(source, -1).wait_recv()
        left = at.column(-1)
        sums[source, left, keys_half] = (
            sums[source, left, keys_half].astype(f32) + h_in[1, source].astype(f32)
        ).astype(bf16)
        x_copy(source, -1).start()

    def merge_across(source):
        x_copy(source, 1).wait_recv()
        x_copy(source, -1).wait_recv()
        sums[source, x] = (
            sums[source, x].astype(f32)
            + x_in[0, source].astype(f32)
            + x_in[1, source].astype(f32)
        ).astype(bf16)
        z_home(source).start()

    for step in range(reach, -2, -1):
        each(step, merge_twin)
        if step == 0:
            for hop in (2, 1, 3):
                column = at.column(hop)
                twin_tile(hop).wait_recv()
                sums[z, column] = (
                    back[z, column, core].astype(f32) + e_in[column].astype(f32)
                ).astype(bf16)
                row_copy(hop).start()
        each(step + 1, merge_half)
        each(step + 2, merge_across)

    total[...] = selfs[...]
    twin_tile(0).wait_recv()
    total[core] += e_in[x].astype(f32)
    for hop in (1, 3, 2):
        row_copy(hop).wait_recv()
        tree = (at.column(-hop) < x).astype(jnp.int32)
        total[tree] += r_in[hop].astype(f32)

    def take(source):
        z_arrival(source).wait_recv()
        tree = (source < z).astype(jnp.int32)
        total[tree] += z_in[source].astype(f32)

    for step in range(reach, 0, -1):
        each(step, take)

    final[...] = total[...].astype(bf16)

    def regroup(step):
        peer = (at.y + step) % heads
        column = pl.ds(pl.multiple_of(at.y * HEAD_DIM, HEAD_DIM), HEAD_DIM)
        rows_k = pl.ds(pl.multiple_of(peer * share, share), share)
        rows_v = pl.ds(pl.multiple_of(BLOCK_TOKENS + peer * share, share), share)
        return (
            remote(final.at[:, rows_k, :], key_out.at[:, :, column],
                   y_send.at[2 * step], y_recv.at[2 * step], at.head_peer(step)),
            remote(final.at[:, rows_v, :], value_out.at[:, :, column],
                   y_send.at[2 * step + 1], y_recv.at[2 * step + 1], at.head_peer(step)),
        )

    for step in range(1, heads):
        for copy in regroup(step):
            copy.start()
    mine = pl.ds(pl.multiple_of(at.y * HEAD_DIM, HEAD_DIM), HEAD_DIM)
    key_out[:, :, mine] = final[:, pl.ds(pl.multiple_of(at.y * share, share), share), :]
    value_out[:, :, mine] = final[
        :, pl.ds(pl.multiple_of(BLOCK_TOKENS + at.y * share, share), share), :
    ]
    for step in range(1, heads):
        for copy in regroup(step):
            copy.wait()

    for step in range(X_CHIPS):
        twin_tile(step).wait_send()
    for hop in (1, 3, 2):
        row_copy(hop).wait_send()

    def drain(source):
        twin_row(source).wait_send()
        for step in (1, -1):
            x_half(source, step).wait_send()
            x_copy(source, step).wait_send()
        z_home(source).wait_send()

    for step in range(1, layers // 2 + 1):
        each(step, drain)


def scatter_tiles(selfs, back, heads, leaves):
    layers = leaves // ROW
    dma = pltpu.SemaphoreType.DMA
    vmem = pl.BlockSpec(memory_space=pltpu.VMEM)
    bf16 = jnp.bfloat16
    share = BLOCK_TOKENS // heads
    out = jax.ShapeDtypeStruct((2, share, heads * HEAD_DIM), bf16)
    return pl.pallas_call(
        functools.partial(scatter_kernel, heads, leaves),
        out_shape=(out, out),
        in_specs=[vmem] * 2,
        out_specs=(vmem, vmem),
        scratch_shapes=[
            pltpu.VMEM((layers, X_CHIPS, KV_ROWS, HEAD_DIM), bf16),
            pltpu.VMEM((layers, X_CHIPS, KV_ROWS, HEAD_DIM), bf16),
            pltpu.VMEM((X_CHIPS, KV_ROWS, HEAD_DIM), bf16),
            pltpu.VMEM((2, layers, KV_ROWS, HEAD_DIM), bf16),
            pltpu.VMEM((2, layers, BLOCK_TOKENS, HEAD_DIM), bf16),
            pltpu.VMEM((X_CHIPS, KV_ROWS, HEAD_DIM), bf16),
            pltpu.VMEM((layers, KV_ROWS, HEAD_DIM), bf16),
            pltpu.VMEM((2, KV_ROWS, HEAD_DIM), jnp.float32),
            pltpu.VMEM((2, KV_ROWS, HEAD_DIM), bf16),
            dma((2 * heads,)), dma((2 * heads,)),
            dma((layers,)), dma((layers,)),
            dma((X_CHIPS,)), dma((X_CHIPS,)),
            dma((2, layers)), dma((2, layers)),
            dma((2, layers)), dma((2, layers)),
            dma((layers,)), dma((layers,)),
            dma((X_CHIPS,)), dma((X_CHIPS,)),
        ],
        compiler_params=pltpu.CompilerParams(
            collective_id=1, has_side_effects=True, vmem_limit_bytes=SCATTER_VMEM
        ),
        cost_estimate=pl.CostEstimate(
            flops=1 << 34, bytes_accessed=8 << 20, transcendentals=0
        ),
        name="scatter_tiles",
    )(selfs, back)


def body(queries, keys, values, output_gradient, parents):
    heads, leaves = lax.axis_size("head"), lax.axis_size("leaf")
    local = jnp.concatenate([keys, values], axis=1)
    own, buf = gather_tiles(parents, local, heads, leaves)
    buf = buf.reshape(leaves, TILE_ROWS, HEAD_DIM)
    query_grads, selfs, back = attend(parents, queries, output_gradient, own, buf)
    back = back.reshape(leaves // ROW, X_CHIPS, 2, KV_ROWS, HEAD_DIM)
    key_gradient, value_gradient = scatter_tiles(selfs, back, heads, leaves)
    return query_grads, key_gradient, value_gradient


def solution(mesh):
    in_specs = (
        P("leaf", None, "head"),
        P("leaf", "head", None),
        P("leaf", "head", None),
        P("leaf", None, "head"),
        P("leaf"),
    )
    out_specs = (P("leaf", None, "head"), P("leaf", "head", None), P("leaf", "head", None))
    return jax.shard_map(body, mesh=mesh, in_specs=in_specs, out_specs=out_specs, check_vma=False)
```
